512 devices in a mesh: gx: 8 (over z), gy: 4 (over x_lo, core), gz: 16 (over y, x_hi).
Axes of the slice: x: 4 (x_hi: 2, x_lo: 2; x = x_hi * 2 + x_lo), y: 8, z: 8, core: 2. Of those that a mesh axis runs over, the one named last changes fastest.
Arguments:
- probe_bits: int32 [32, 128, 512], P('gx', 'gz', 'gy'), may hold values from -2147483648 to 2147483646
- disorder_levels: int32 [32, 128, 512], P('gx', 'gz', 'gy'), may hold values from -2147483648 to 2147483647, as said below
Outputs:
- moments: float32 [3, 8], replicated
- previous: float32 [8, 32, 512, 512], P(None, 'gx', 'gz', 'gy')
- current: float32 [8, 32, 512, 512], P(None, 'gx', 'gz', 'gy')
The draws below stay inside these ranges and needn't reach their ends.
Inputs may be any that keep to these rules, and one draw needn't show every extreme that they name: `disorder_levels`: every byte of a word is a level 0 to 255.
All inputs are finite; a program needn't handle non-finite values.
Results may differ from the reference program's by a relative error of at most 0.00002.
Values sent between devices are 32-bit elements; how exact they have to be, the bound alone decides.
A program may use at most 64 MiB of HBM per device.

```python
import jax
import jax.numpy as jnp
from jax import lax

PROBES = 8
LEVELS = 256
NX = 32
NY = 512
NZ = 512
NSITES = 8388608


def draw_disorder_levels(key, part):
    shape = (NX, NZ, NY)
    group = jax.random.randint(jax.random.fold_in(key, 11), (), 0, 2)
    base = 32 + jax.random.randint(jax.random.fold_in(key, 12), (), 0, 64) + 128 * group
    slope = 32 * (2 * jax.random.randint(jax.random.fold_in(key, 13), (), 0, 2) - 1)
    offsets = jax.random.randint(jax.random.fold_in(key, 14), (4, 4, 4), -16, 17)
    widths = jax.random.randint(jax.random.fold_in(key, 15), (4, 4, 4), 16, 80)
    patch_x = lax.broadcasted_iota(jnp.int32, shape, 0) * 4 // NX
    patch_z = lax.broadcasted_iota(jnp.int32, shape, 1) * 4 // NZ
    patch_y = lax.broadcasted_iota(jnp.int32, shape, 2) * 4 // NY
    local_offset = offsets[patch_x, patch_z, patch_y]
    local_width = widths[patch_x, patch_z, patch_y]
    centre = base + slope * (patch_x - 1) + local_offset
    raw = jax.random.randint(jax.random.fold_in(key, 16), shape, 0, 161)
    jitter = raw % (2 * local_width + 1) - local_width
    patchy = jnp.clip(centre + jitter, 0, LEVELS - 1)
    background = jax.random.randint(jax.random.fold_in(key, 17), shape, 0, LEVELS)
    picker = jax.random.randint(jax.random.fold_in(key, 18), shape, 0, 8)
    levels = jnp.where(picker == 0, background, patchy).astype(jnp.int32)
    grouped = levels.reshape(NX, NZ // 4, 4, NY)
    top_byte = grouped[:, :, 3, :]
    top_signed = jnp.where(top_byte >= 128, top_byte - 256, top_byte)
    packed = grouped[:, :, 0, :] + grouped[:, :, 1, :] * 256 + grouped[:, :, 2, :] * 65536 + top_signed * 16777216
    return packed.astype(jnp.int32)


def plant(entries, rng, low, top_value):
    shape = entries.shape
    place = [jax.random.randint(jax.random.fold_in(rng, axis), (), 0, shape[axis]) for axis in range(len(shape))]
    entries = entries.at[tuple(place)].set(low)
    longest = shape.index(max(shape))
    place[longest] = (place[longest] + 1) % shape[longest]
    return entries.at[tuple(place)].set(top_value)


def shard_levels(stream_key, extent, cuts, smallest, top_value):
    factor_of, own = 1.0, jax.random.fold_in(stream_key, 6)
    for axis_at, parts in cuts:
        heights = jnp.exp(jax.random.uniform(jax.random.fold_in(own, axis_at), (parts,), jnp.float32, smallest / len(cuts), top_value / len(cuts)))
        factor_of = factor_of * jnp.repeat(heights, extent[axis_at] // parts).reshape([-1 if axis == axis_at else 1 for axis in range(len(extent))])
    return factor_of


def setup_inputs(seed: int = 0) -> dict:
    seeds = jax.random.split(jax.random.key(seed), 3)
    probe_bits = plant(jax.random.randint(seeds[0], (NX, NZ // 4, NY), -2147483648, 2147483647), jax.random.fold_in(seeds[0], 1), -2147483648, 2147483646).astype(jnp.int32)
    disorder_levels = draw_disorder_levels(jax.random.fold_in(seeds[2], 71), 0)
    return dict(probe_bits=probe_bits, disorder_levels=disorder_levels)


disorder_width = 4.0
spectral_scale = 8.4


def unpack_signs(packed):
    shifts = 4 * jnp.arange(PROBES, dtype=jnp.int32)[:, None] + jnp.arange(4, dtype=jnp.int32)[None, :]
    bit_values = jnp.right_shift(packed[None, :, :, None, :], shifts[:, None, None, :, None]) & 1
    layout = bit_values.shape
    flat = bit_values.reshape(layout[0], layout[1], layout[2] * layout[3], layout[4])
    return 2.0 * flat.astype(jnp.float32) - 1.0


def unpack_energy(packed):
    shifts = 8 * jnp.arange(4, dtype=jnp.int32)
    levels = jnp.right_shift(packed[:, :, None, :], shifts[None, None, :, None]) & 255
    layout = levels.shape
    flat = levels.reshape(layout[0], layout[1] * layout[2], layout[3])
    return disorder_width * ((flat.astype(jnp.float32) + 0.5) / LEVELS - 0.5)


def apply_ham(field, energy):
    beside = jnp.roll(field, -1, 1) + jnp.roll(field, 1, 1)
    beside = beside + jnp.roll(field, -1, 3) + jnp.roll(field, 1, 3)
    beside = beside + jnp.roll(field, -1, 2) + jnp.roll(field, 1, 2)
    return (energy[None] * field - beside) / spectral_scale


def reference(probe_bits, disorder_levels):
    signs = unpack_signs(probe_bits)
    energy = unpack_energy(disorder_levels)
    first = apply_ham(signs, energy)
    second = 2.0 * apply_ham(first, energy) - signs
    third = 2.0 * apply_ham(second, energy) - first
    moments = jnp.stack([jnp.sum(signs * vec, axis=(1, 2, 3)) for vec in (first, second, third)]) / NSITES
    return moments, second, third
```

```python
import jax
import jax.numpy as jnp
from jax import lax
from jax.experimental import pallas as pl
from jax.experimental.pallas import tpu as pltpu
from jax.sharding import PartitionSpec as P

F32 = jnp.float32
I32 = jnp.int32
MESH = pl.DeviceIdType.MESH
C1 = 1.0 / 8.4
C2 = 2.0 / 8.4
SIZES = {"gx": 8, "gy": 4, "gz": 16}
NSITES = 32 * 512 * 512
LOCAL = 4 * 32 * 128

DIRS = sorted(
    [
        (dx, dy, dz)
        for dx in (-1, 0, 1)
        for dy in (-1, 0, 1)
        for dz in (-1, 0, 1)
        if (dx, dy, dz) != (0, 0, 0)
    ],
    key=lambda d: (-abs(d[2]), abs(d[0]) + abs(d[1])),
)


def srl(a, n):
    return lax.shift_right_logical(a, n if hasattr(n, "shape") and n.shape == a.shape else jnp.full(a.shape, n, I32))


def roll(a, n, axis):
    return pltpu.roll(a, n % a.shape[axis], axis)


def count_bits(a, b, c, d, e, f):
    x = a ^ b
    s1 = x ^ c
    c1 = (a & b) | (c & x)
    y = d ^ e
    s2 = y ^ f
    c2 = (d & e) | (f & y)
    h = s1 & s2
    z = c1 ^ c2
    return s1 ^ s2, z ^ h, (c1 & c2) | (h & z)


def nibbles(planes, word, shift):
    ones = 0x11111111
    p0, p1, p2 = planes
    return (
        (srl(p0, shift) & ones)
        | ((srl(p1, shift) & ones) << 1)
        | ((srl(p2, shift) & ones) << 2)
        | ((srl(word, shift) & ones) << 3)
    )


def kernel(
    bits_hbm, dis_hbm, mom, prev, cur,
    E, NM, NZ1, NZ2, NY, NY2,
    EPM, EMM, E2M, EPZ1, EMZ1, EPZ2, EMZ2, E2Z, EPY, EMY, E2Y, EPY2, EMY2,
    V1M, V1Z1, V1Z2, V1Y, V1YI, V1Y2I, V1Y2, V2M, V2Z, V2YI, ACC, S, G,
    in_sem, hs, hr, rs, rr,
):
    gx, gy, gz = lax.axis_index("gx"), lax.axis_index("gy"), lax.axis_index("gz")
    yy, xhi = gz // 2, lax.rem(gz, 2)

    own_copies = [
        pltpu.make_async_copy(src, E.at[a, 1, 3:7, 0:8, :], in_sem.at[a])
        for a, src in enumerate((bits_hbm, dis_hbm))
    ]
    for cp in own_copies:
        cp.start()

    def neighbour(d):
        return {
            "gx": lax.rem(gx + d[0] + 8, 8),
            "gy": lax.rem(gy + d[1] + 4, 4),
            "gz": lax.rem(gz + d[2] + 16, 16),
        }

    x8 = xhi * 4 + gy

    def peer(phase, k):
        if phase == 0:
            t = lax.rem(x8 + k, 8)
            return {"gx": gx, "gy": lax.rem(t, 4), "gz": yy * 2 + t // 4}
        if phase == 1:
            return {"gx": lax.rem(gx + k, 8), "gy": gy, "gz": gz}
        return {"gx": gx, "gy": gy, "gz": lax.rem(yy + k, 8) * 2 + xhi}

    ranks = (x8, gx, yy)

    barrier = pltpu.get_barrier_semaphore()
    n_sig = 0
    for d in DIRS:
        pl.semaphore_signal(barrier, inc=1, device_id=neighbour(d), device_id_type=MESH)
        n_sig += 1
    for phase in range(3):
        for k in range(1, 8):
            pl.semaphore_signal(barrier, inc=1, device_id=peer(phase, k), device_id_type=MESH)
            n_sig += 1

    lane = lax.broadcasted_iota(I32, (8, 128), 1)
    row = lax.broadcasted_iota(I32, (8, 128), 0)
    l0, l127 = lane == 0, lane == 127
    r0, r7 = row == 0, row == 7

    for cp in own_copies:
        cp.wait()
    pl.semaphore_wait(barrier, n_sig)

    halo = []
    for i, (dx, dy, dz) in enumerate(DIRS):
        n = 3 - abs(dy) - abs(dz)
        if dx == 1:
            xs, xd = slice(7 - n, 7), slice(3 - n, 3)
        elif dx == -1:
            xs, xd = slice(3, 3 + n), slice(7, 7 + n)
        else:
            xs, xd = slice(3, 7), slice(3, 7)
        if dz == 1:
            ws, wd = slice(7, 8), slice(15, 16)
        elif dz == -1:
            ws, wd = slice(0, 1), slice(8, 9)
        else:
            ws, wd = slice(0, 8), slice(0, 8)
        cp = pltpu.make_async_remote_copy(
            src_ref=E.at[:, 1, xs, ws, :],
            dst_ref=E.at[:, 1 - dy, xd, wd, :],
            send_sem=hs.at[i],
            recv_sem=hr.at[i],
            device_id=neighbour((dx, dy, dz)),
            device_id_type=MESH,
        )
        cp.start()
        halo.append(cp)
    for cp in halo:
        cp.wait_recv()

    def tile(a, t, xi, second):
        return E[a, t, xi + 1, (8 if second else 0) : (16 if second else 8), :]

    def pack_y(a, second):
        out = jnp.zeros((8, 128), I32)
        for xi in range(8):
            left, own, right = (tile(a, t, xi, second) for t in range(3))
            m1 = jnp.where(lane >= 64, left, own)
            m2 = jnp.where(lane >= 64, own, right)
            slot = lane - 16 * xi
            out = jnp.where((slot >= 0) & (slot < 8), roll(m1, 16 * xi - 125, 1), out)
            out = jnp.where((slot >= 8) & (slot < 16), roll(m2, 16 * xi + 8 - 126, 1), out)
        return out

    def up_down(main, second):
        up = roll(jnp.where(r0, second, main), 7, 0)
        down = roll(jnp.where(r7, second, main), 1, 0)
        return up, down

    def z_words(word, up, down):
        zp = (srl(word, 1) & 0x77777777) | (up << 3 & -0x77777778)
        zm = (word << 1 & -0x11111112) | (srl(down, 3) & 0x11111111)
        return zp, zm

    def sides(a, xi, second):
        left, own, right = (tile(a, t, xi, second) for t in range(3))
        return roll(jnp.where(l127, left, own), 1, 1), roll(jnp.where(l0, right, own), 127, 1)

    def energy(word, shift):
        return ((srl(word, shift) & 255).astype(F32) + 0.5) * (1.0 / 64.0) - 2.0

    def zshift(depth, unit):
        return jnp.where(row < 4, unit * (depth - 1), unit * (4 - depth))

    for xi in range(8):
        main, second = tile(0, 1, xi, False), tile(0, 1, xi, True)
        up, down = up_down(main, second)
        zp, zm = z_words(main, up, down)
        ym, yp = sides(0, xi, False)
        planes = count_bits(tile(0, 1, xi + 1, False), tile(0, 1, xi - 1, False), yp, ym, zp, zm)
        for j in range(4):
            NM[xi, j] = nibbles(planes, main, j)
            e = energy(tile(1, 1, xi, False), 8 * j)
            EPM[xi, j] = (6.0 + e) * C1
            EMM[xi, j] = (6.0 - e) * C1
            E2M[xi, j] = e * C2
        if 1 <= xi <= 6:
            up, down = up_down(second, main)
            zp, zm = z_words(second, up, down)
            ym, yp = sides(0, xi, True)
            planes = count_bits(tile(0, 1, xi + 1, True), tile(0, 1, xi - 1, True), yp, ym, zp, zm)
            NZ1[xi - 1] = nibbles(planes, second, zshift(1, 1))
            e = energy(tile(1, 1, xi, True), zshift(1, 8))
            EPZ1[xi - 1] = (6.0 + e) * C1
            EMZ1[xi - 1] = (6.0 - e) * C1
            if 2 <= xi <= 5:
                E2Z[xi - 2] = e * C2
                NZ2[xi - 2] = nibbles(planes, second, zshift(2, 1))
                e = energy(tile(1, 1, xi, True), zshift(2, 8))
                EPZ2[xi - 2] = (6.0 + e) * C1
                EMZ2[xi - 2] = (6.0 - e) * C1

    yw, yw2 = pack_y(0, False), pack_y(0, True)
    yd, yd2 = pack_y(1, False), pack_y(1, True)

    def y_planes(word, up, down):
        zp, zm = z_words(word, up, down)
        return count_bits(roll(word, 1, 1), roll(word, 127, 1), roll(word, 16, 1), roll(word, 112, 1), zp, zm)

    planes = y_planes(yw, *up_down(yw, yw2))
    for j in range(4):
        NY[j] = nibbles(planes, yw, j)
        e = energy(yd, 8 * j)
        EPY[j] = (6.0 + e) * C1
        EMY[j] = (6.0 - e) * C1
        E2Y[j] = e * C2
    planes = y_planes(yw2, *up_down(yw2, yw))
    NY2[...] = nibbles(planes, yw2, zshift(1, 1))
    e = energy(yd2, zshift(1, 8))
    EPY2[...] = (6.0 + e) * C1
    EMY2[...] = (6.0 - e) * C1

    col = lane & 15

    def inner(y):
        return jnp.where(col == 3, roll(y, 121, 1), y)

    def first_order(word, ep, em, sh):
        t = srl(word, sh)
        return jnp.where((t & 8) != 0, ep, em) - C2 * (t & 7).astype(F32)

    def sign(word, sh):
        return jnp.where((srl(word, sh) & 8) != 0, 1.0, -1.0).astype(F32)

    def around(get, edge, ins, xi, j, sub):
        c = get(xi, j)
        a = roll(ins, 127 - (16 * xi + 2), 1)
        s = get(xi + 1, j) + get(xi - 1, j)
        s = s + roll(jnp.where(l127, a, c), 1, 1) + roll(jnp.where(l0, a, c), 127, 1)
        zp = get(xi, j + 1) if j < 3 else roll(jnp.where(r0, edge(xi), get(xi, 0)), 7, 0)
        zm = get(xi, j - 1) if j > 0 else roll(jnp.where(r7, edge(xi), get(xi, 3)), 1, 0)
        return c, s + (zp + zm)

    def second_main(r, xi, j):
        c, s = around(
            lambda x, k: V1M[r, x, k], lambda x: V1Z1[r, x - 1], V1YI[r, j], xi, j, None
        )
        sg = sign(NM[xi, j], 4 * r)
        return c, sg, E2M[xi, j] * c - C2 * s - sg

    def pass_a(r, carry):
        sh = 4 * r
        for xi in range(8):
            for j in range(4):
                V1M[r, xi, j] = first_order(NM[xi, j], EPM[xi, j], EMM[xi, j], sh)
        for xi in range(6):
            V1Z1[r, xi] = first_order(NZ1[xi], EPZ1[xi], EMZ1[xi], sh)
        for xi in range(4):
            V1Z2[r, xi] = first_order(NZ2[xi], EPZ2[xi], EMZ2[xi], sh)
        for j in range(4):
            y = first_order(NY[j], EPY[j], EMY[j], sh)
            V1Y[r, j] = y
            V1YI[r, j] = inner(y)
        y = first_order(NY2[...], EPY2[...], EMY2[...], sh)
        V1Y2[r] = y
        V1Y2I[r] = inner(y)
        a1 = jnp.zeros((8, 128), F32)
        a2 = jnp.zeros((8, 128), F32)
        a3 = jnp.zeros((8, 128), F32)
        for x in range(4):
            for j in range(4):
                v1, sg, v2 = second_main(r, x + 2, j)
                V2M[r, x + 1, j] = v2
                prev[r, x, pl.ds(j, 8, stride=4), :] = v2
                a1 = a1 + sg * v1
                a2 = a2 + v1 * v1
                a3 = a3 + v1 * v2
        a3 = 2.0 * a3 - a1
        a2 = 2.0 * a2 - float(LOCAL // 1024)
        for m, acc in enumerate((a1, a2, a3)):
            ACC[m, pl.ds(r, 1), :] = jnp.sum(acc, axis=0, keepdims=True)
        return carry

    lax.fori_loop(0, 8, pass_a, 0)

    mine = jnp.zeros((8, 128), F32)
    for m in range(3):
        tot = jnp.sum(ACC[m], axis=1, keepdims=True)
        mine = mine + jnp.where(lane == row + 8 * m, jnp.broadcast_to(tot, (8, 128)), 0.0)

    def sum_rows(t):
        t = t + roll(t, 4, 0)
        t = t + roll(t, 2, 0)
        return t + roll(t, 1, 0)

    mine = sum_rows(mine)

    def send(phase, value):
        S[phase] = value
        copies = []
        for k in range(1, 8):
            cp = pltpu.make_async_remote_copy(
                src_ref=S.at[phase, 0:1, :],
                dst_ref=G.at[phase, pl.ds(ranks[phase], 1), :],
                send_sem=rs.at[phase, k],
                recv_sem=rr.at[phase, k],
                device_id=peer(phase, k),
                device_id_type=MESH,
            )
            cp.start()
            copies.append(cp)
        return copies

    def collect(phase, copies, value):
        for cp in copies:
            cp.wait_recv()
        return sum_rows(jnp.where(row == ranks[phase], value, G[phase]))

    sends0 = send(0, mine)

    def pass_b(r, carry):
        for xi, slot in ((1, 0), (6, 5)):
            for j in range(4):
                V2M[r, slot, j] = second_main(r, xi, j)[2]
        for x in range(4):
            xi = x + 2
            c = V1Z1[r, xi - 1]
            a = roll(V1Y2I[r], 127 - (16 * xi + 2), 1)
            s = V1Z1[r, xi] + V1Z1[r, xi - 2]
            s = s + roll(jnp.where(l127, a, c), 1, 1) + roll(jnp.where(l0, a, c), 127, 1)
            ins = jnp.where(r7, roll(V1M[r, xi, 0], 7, 0), roll(V1M[r, xi, 3], 1, 0))
            s = s + (V1Z2[r, x] + ins)
            V2Z[r, x] = E2Z[x] * c - C2 * s - sign(NZ1[xi - 1], 4 * r)
        for j in range(4):
            c = V1Y[r, j]
            s = roll(c, 1, 1) + roll(c, 127, 1) + (roll(c, 16, 1) + roll(c, 112, 1))
            zp = V1Y[r, j + 1] if j < 3 else roll(jnp.where(r0, V1Y2[r], V1Y[r, 0]), 7, 0)
            zm = V1Y[r, j - 1] if j > 0 else roll(jnp.where(r7, V1Y2[r], V1Y[r, 3]), 1, 0)
            s = s + (zp + zm)
            V2YI[r, j] = inner(E2Y[j] * c - C2 * s - sign(NY[j], 4 * r))
        return carry

    lax.fori_loop(0, 8, pass_b, 0)
    total = collect(0, sends0, mine)
    sends1 = send(1, total)

    def pass_c(r, carry):
        for x in range(4):
            for j in range(4):
                c, s = around(
                    lambda xi, k: V2M[r, xi - 1, k], lambda xi: V2Z[r, xi - 2], V2YI[r, j], x + 2, j, None
                )
                cur[r, x, pl.ds(j, 8, stride=4), :] = E2M[x + 2, j] * c - C2 * s - V1M[r, x + 2, j]
        return carry

    lax.fori_loop(0, 8, pass_c, 0)
    total1 = collect(1, sends1, total)
    sends2 = send(2, total1)
    total2 = collect(2, sends2, total1) * (1.0 / NSITES)
    out = jnp.where(r0, total2, jnp.where(row == 1, roll(total2, 120, 1), roll(total2, 112, 1)))
    mom[...] = out[:3, :8]
    for cp in halo + sends0 + sends1 + sends2:
        cp.wait_send()


def vm(*shape, dtype=F32):
    return pltpu.VMEM(shape + (8, 128), dtype)


def per_device(probe_bits, disorder_levels):
    dma = pltpu.SemaphoreType.DMA
    return pl.pallas_call(
        kernel,
        out_shape=(
            jax.ShapeDtypeStruct((3, 8), F32),
            jax.ShapeDtypeStruct((8, 4, 32, 128), F32),
            jax.ShapeDtypeStruct((8, 4, 32, 128), F32),
        ),
        in_specs=[pl.BlockSpec(memory_space=pltpu.HBM)] * 2,
        out_specs=(pl.BlockSpec(memory_space=pltpu.VMEM),) * 3,
        scratch_shapes=[
            pltpu.VMEM((2, 3, 10, 16, 128), I32),
            vm(8, 4, dtype=I32), vm(6, dtype=I32), vm(4, dtype=I32), vm(4, dtype=I32), vm(dtype=I32),
            vm(8, 4), vm(8, 4), vm(8, 4),
            vm(6), vm(6), vm(4), vm(4), vm(4),
            vm(4), vm(4), vm(4), vm(), vm(),
            vm(8, 8, 4), vm(8, 6), vm(8, 4), vm(8, 4), vm(8, 4), vm(8), vm(8),
            vm(8, 6, 4), vm(8, 4), vm(8, 4),
            vm(3), vm(3), vm(3),
            dma((2,)), dma((26,)), dma((26,)), dma((3, 8)), dma((3, 8)),
        ],
        compiler_params=pltpu.CompilerParams(
            collective_id=0, has_side_effects=True, vmem_limit_bytes=24 * 1024 * 1024
        ),
    )(pltpu.with_memory_space_constraint(probe_bits, pltpu.HBM), pltpu.with_memory_space_constraint(disorder_levels, pltpu.HBM))


def solution(mesh):
    return jax.shard_map(
        per_device,
        mesh=mesh,
        in_specs=(P("gx", "gz", "gy"), P("gx", "gz", "gy")),
        out_specs=(P(), P(None, "gx", "gz", "gy"), P(None, "gx", "gz", "gy")),
        check_vma=False,
    )
```

```python
import jax
import jax.numpy as jnp
from jax import lax
from jax.experimental import pallas as pl
from jax.experimental.pallas import tpu as pltpu
from jax.sharding import PartitionSpec as P

F32 = jnp.float32
I32 = jnp.int32
MESH = pl.DeviceIdType.MESH
C1 = 1.0 / 8.4
C2 = 2.0 / 8.4
SIZES = {"gx": 8, "gy": 4, "gz": 16}
NSITES = 32 * 512 * 512
LOCAL = 4 * 32 * 128

DIRS = sorted(
    [
        (dx, dy, dz)
        for dx in (-1, 0, 1)
        for dy in (-1, 0, 1)
        for dz in (-1, 0, 1)
        if (dx, dy, dz) != (0, 0, 0)
    ],
    key=lambda d: (-abs(d[2]), abs(d[0]) + abs(d[1])),
)


def srl(a, n):
    return lax.shift_right_logical(a, n if hasattr(n, "shape") and n.shape == a.shape else jnp.full(a.shape, n, I32))


def roll(a, n, axis):
    return pltpu.roll(a, n % a.shape[axis], axis)


def count_bits(a, b, c, d, e, f):
    x = a ^ b
    s1 = x ^ c
    c1 = (a & b) | (c & x)
    y = d ^ e
    s2 = y ^ f
    c2 = (d & e) | (f & y)
    h = s1 & s2
    z = c1 ^ c2
    return s1 ^ s2, z ^ h, (c1 & c2) | (h & z)


def nibbles(planes, word, shift):
    ones = 0x11111111
    p0, p1, p2 = planes
    return (
        (srl(p0, shift) & ones)
        | ((srl(p1, shift) & ones) << 1)
        | ((srl(p2, shift) & ones) << 2)
        | ((srl(word, shift) & ones) << 3)
    )


def kernel(
    bits_hbm, dis_hbm, mom, prev, cur,
    E, NM, NZ1, NZ2, NY, NY2,
    EPM, EMM, E2M, EPZ1, EMZ1, EPZ2, EMZ2, E2Z, EPY, EMY, E2Y, EPY2, EMY2,
    V1M, V1Z1, V1Z2, V1Y, V1YI, V1Y2I, V1Y2, V2M, V2Z, V2YI, ACC, S, GP, GL,
    in_sem, hs, hr, ps, pr, ls, lr,
):
    gx, gy, gz = lax.axis_index("gx"), lax.axis_index("gy"), lax.axis_index("gz")
    yy, xhi = gz // 2, lax.rem(gz, 2)

    own_copies = [
        pltpu.make_async_copy(src, E.at[a, 1, 3:7, 0:8, :], in_sem.at[a])
        for a, src in enumerate((bits_hbm, dis_hbm))
    ]
    for cp in own_copies:
        cp.start()

    def neighbour(d):
        return {
            "gx": lax.rem(gx + d[0] + 8, 8),
            "gy": lax.rem(gy + d[1] + 4, 4),
            "gz": lax.rem(gz + d[2] + 16, 16),
        }

    core = lax.rem(gy, 2)
    px = xhi * 2 + gy // 2
    place = yy * 4 + px

    def plane_peer(k, c):
        t = lax.rem(place + k, 32)
        q = lax.rem(t, 4)
        return {"gx": gx, "gy": lax.rem(q, 2) * 2 + c, "gz": (t // 4) * 2 + q // 2}

    def line_peer(k, c):
        return {"gx": lax.rem(gx + k, 8), "gy": (gy // 2) * 2 + c, "gz": gz}

    barrier = pltpu.get_barrier_semaphore()

    def greet(device):
        pl.semaphore_signal(barrier, inc=1, device_id=device, device_id_type=MESH)

    for d in DIRS:
        greet(neighbour(d))
    for k in range(1, 8):
        greet(line_peer(k, 1))

    @pl.when(core == 0)
    def _():
        greet(line_peer(0, 1))

    @pl.when(core == 1)
    def _():
        for k in range(1, 32):
            greet(plane_peer(k, 1))
        for k in range(32):
            greet(plane_peer(k, 0))

    lane = lax.broadcasted_iota(I32, (8, 128), 1)
    row = lax.broadcasted_iota(I32, (8, 128), 0)
    l0, l127 = lane == 0, lane == 127
    r0, r7 = row == 0, row == 7

    for cp in own_copies:
        cp.wait()

    @pl.when(core == 0)
    def _():
        pl.semaphore_wait(barrier, 26 + 32)

    @pl.when(core == 1)
    def _():
        pl.semaphore_wait(barrier, 26 + 31 + 15)


    halo = []
    for i, (dx, dy, dz) in enumerate(DIRS):
        n = 3 - abs(dy) - abs(dz)
        if dx == 1:
            xs, xd = slice(7 - n, 7), slice(3 - n, 3)
        elif dx == -1:
            xs, xd = slice(3, 3 + n), slice(7, 7 + n)
        else:
            xs, xd = slice(3, 7), slice(3, 7)
        if dz == 1:
            ws, wd = slice(7, 8), slice(15, 16)
        elif dz == -1:
            ws, wd = slice(0, 1), slice(8, 9)
        else:
            ws, wd = slice(0, 8), slice(0, 8)
        cp = pltpu.make_async_remote_copy(
            src_ref=E.at[:, 1, xs, ws, :],
            dst_ref=E.at[:, 1 - dy, xd, wd, :],
            send_sem=hs.at[i],
            recv_sem=hr.at[i],
            device_id=neighbour((dx, dy, dz)),
            device_id_type=MESH,
        )
        cp.start()
        halo.append(cp)
    for cp in halo:
        cp.wait_recv()

    def tile(a, t, xi, second):
        return E[a, t, xi + 1, (8 if second else 0) : (16 if second else 8), :]

    def pack_y(a, second):
        out = jnp.zeros((8, 128), I32)
        for xi in range(8):
            left, own, right = (tile(a, t, xi, second) for t in range(3))
            m1 = jnp.where(lane >= 64, left, own)
            m2 = jnp.where(lane >= 64, own, right)
            slot = lane - 16 * xi
            out = jnp.where((slot >= 0) & (slot < 8), roll(m1, 16 * xi - 125, 1), out)
            out = jnp.where((slot >= 8) & (slot < 16), roll(m2, 16 * xi + 8 - 126, 1), out)
        return out

    def up_down(main, second):
        up = roll(jnp.where(r0, second, main), 7, 0)
        down = roll(jnp.where(r7, second, main), 1, 0)
        return up, down

    def z_words(word, up, down):
        zp = (srl(word, 1) & 0x77777777) | (up << 3 & -0x77777778)
        zm = (word << 1 & -0x11111112) | (srl(down, 3) & 0x11111111)
        return zp, zm

    def sides(a, xi, second):
        left, own, right = (tile(a, t, xi, second) for t in range(3))
        return roll(jnp.where(l127, left, own), 1, 1), roll(jnp.where(l0, right, own), 127, 1)

    def energy(word, shift):
        return ((srl(word, shift) & 255).astype(F32) + 0.5) * (1.0 / 64.0) - 2.0

    def zshift(depth, unit):
        return jnp.where(row < 4, unit * (depth - 1), unit * (4 - depth))

    for xi in range(8):
        main, second = tile(0, 1, xi, False), tile(0, 1, xi, True)
        up, down = up_down(main, second)
        zp, zm = z_words(main, up, down)
        ym, yp = sides(0, xi, False)
        planes = count_bits(tile(0, 1, xi + 1, False), tile(0, 1, xi - 1, False), yp, ym, zp, zm)
        for j in range(4):
            NM[xi, j] = nibbles(planes, main, j)
            e = energy(tile(1, 1, xi, False), 8 * j)
            EPM[xi, j] = (6.0 + e) * C1
            EMM[xi, j] = (6.0 - e) * C1
            E2M[xi, j] = e * C2
        if 1 <= xi <= 6:
            up, down = up_down(second, main)
            zp, zm = z_words(second, up, down)
            ym, yp = sides(0, xi, True)
            planes = count_bits(tile(0, 1, xi + 1, True), tile(0, 1, xi - 1, True), yp, ym, zp, zm)
            NZ1[xi - 1] = nibbles(planes, second, zshift(1, 1))
            e = energy(tile(1, 1, xi, True), zshift(1, 8))
            EPZ1[xi - 1] = (6.0 + e) * C1
            EMZ1[xi - 1] = (6.0 - e) * C1
            if 2 <= xi <= 5:
                E2Z[xi - 2] = e * C2
                NZ2[xi - 2] = nibbles(planes, second, zshift(2, 1))
                e = energy(tile(1, 1, xi, True), zshift(2, 8))
                EPZ2[xi - 2] = (6.0 + e) * C1
                EMZ2[xi - 2] = (6.0 - e) * C1

    yw, yw2 = pack_y(0, False), pack_y(0, True)
    yd, yd2 = pack_y(1, False), pack_y(1, True)

    def y_planes(word, up, down):
        zp, zm = z_words(word, up, down)
        return count_bits(roll(word, 1, 1), roll(word, 127, 1), roll(word, 16, 1), roll(word, 112, 1), zp, zm)

    planes = y_planes(yw, *up_down(yw, yw2))
    for j in range(4):
        NY[j] = nibbles(planes, yw, j)
        e = energy(yd, 8 * j)
        EPY[j] = (6.0 + e) * C1
        EMY[j] = (6.0 - e) * C1
        E2Y[j] = e * C2
    planes = y_planes(yw2, *up_down(yw2, yw))
    NY2[...] = nibbles(planes, yw2, zshift(1, 1))
    e = energy(yd2, zshift(1, 8))
    EPY2[...] = (6.0 + e) * C1
    EMY2[...] = (6.0 - e) * C1

    col = lane & 15

    def inner(y):
        return jnp.where(col == 3, roll(y, 121, 1), y)

    def first_order(word, ep, em, sh):
        t = srl(word, sh)
        return jnp.where((t & 8) != 0, ep, em) - C2 * (t & 7).astype(F32)

    def sign(word, sh):
        return jnp.where((srl(word, sh) & 8) != 0, 1.0, -1.0).astype(F32)

    def around(get, edge, ins, xi, j, sub):
        c = get(xi, j)
        a = roll(ins, 127 - (16 * xi + 2), 1)
        s = get(xi + 1, j) + get(xi - 1, j)
        s = s + roll(jnp.where(l127, a, c), 1, 1) + roll(jnp.where(l0, a, c), 127, 1)
        zp = get(xi, j + 1) if j < 3 else roll(jnp.where(r0, edge(xi), get(xi, 0)), 7, 0)
        zm = get(xi, j - 1) if j > 0 else roll(jnp.where(r7, edge(xi), get(xi, 3)), 1, 0)
        return c, s + (zp + zm)

    def second_main(r, xi, j):
        c, s = around(
            lambda x, k: V1M[r, x, k], lambda x: V1Z1[r, x - 1], V1YI[r, j], xi, j, None
        )
        sg = sign(NM[xi, j], 4 * r)
        return c, sg, E2M[xi, j] * c - C2 * s - sg

    def pass_a(r, carry):
        sh = 4 * r
        for xi in range(8):
            for j in range(4):
                V1M[r, xi, j] = first_order(NM[xi, j], EPM[xi, j], EMM[xi, j], sh)
        for xi in range(6):
            V1Z1[r, xi] = first_order(NZ1[xi], EPZ1[xi], EMZ1[xi], sh)
        for xi in range(4):
            V1Z2[r, xi] = first_order(NZ2[xi], EPZ2[xi], EMZ2[xi], sh)
        for j in range(4):
            y = first_order(NY[j], EPY[j], EMY[j], sh)
            V1Y[r, j] = y
            V1YI[r, j] = inner(y)
        y = first_order(NY2[...], EPY2[...], EMY2[...], sh)
        V1Y2[r] = y
        V1Y2I[r] = inner(y)
        a1 = jnp.zeros((8, 128), F32)
        a2 = jnp.zeros((8, 128), F32)
        a3 = jnp.zeros((8, 128), F32)
        for x in range(4):
            for j in range(4):
                v1, sg, v2 = second_main(r, x + 2, j)
                V2M[r, x + 1, j] = v2
                prev[r, x, pl.ds(j, 8, stride=4), :] = v2
                a1 = a1 + sg * v1
                a2 = a2 + v1 * v1
                a3 = a3 + v1 * v2
        a3 = 2.0 * a3 - a1
        a2 = 2.0 * a2 - float(LOCAL // 1024)
        for m, acc in enumerate((a1, a2, a3)):
            ACC[m, pl.ds(r, 1), :] = jnp.sum(acc, axis=0, keepdims=True)
        return carry

    lax.fori_loop(0, 8, pass_a, 0)

    mine = jnp.zeros((8, 128), F32)
    for m in range(3):
        tot = jnp.sum(ACC[m], axis=1, keepdims=True)
        mine = mine + jnp.where(lane == row + 8 * m, jnp.broadcast_to(tot, (8, 128)), 0.0)

    def sum_rows(t):
        t = t + roll(t, 4, 0)
        t = t + roll(t, 2, 0)
        return t + roll(t, 1, 0)

    mine = sum_rows(mine)

    slot = place * 2 + core

    def plane_copy(k):
        return pltpu.make_async_remote_copy(
            src_ref=S.at[0, 0:1, :],
            dst_ref=GP.at[pl.ds(slot, 1), :],
            send_sem=ps.at[k],
            recv_sem=pr.at[(1 - core) * 32 + k],
            device_id=plane_peer(k, 1),
            device_id_type=MESH,
        )

    def line_copy(k, c):
        return pltpu.make_async_remote_copy(
            src_ref=S.at[1, 0:1, :],
            dst_ref=GL.at[pl.ds(gx, 1), :],
            send_sem=ls.at[c * 8 + k],
            recv_sem=lr.at[c * 8 + k],
            device_id=line_peer(k, c),
            device_id_type=MESH,
        )

    def plane_arrived(q):
        return pltpu.make_async_remote_copy(
            src_ref=S.at[0, 0:1, :],
            dst_ref=GP.at[0:1, :],
            send_sem=ps.at[0],
            recv_sem=pr.at[q],
            device_id=plane_peer(1, 1),
            device_id_type=MESH,
        ).wait_recv()

    S[0] = mine
    for k in range(1, 32):
        plane_copy(k).start()

    @pl.when(core == 0)
    def _():
        plane_copy(0).start()


    def pass_b(r, carry):
        for xi, slot in ((1, 0), (6, 5)):
            for j in range(4):
                V2M[r, slot, j] = second_main(r, xi, j)[2]
        for x in range(4):
            xi = x + 2
            c = V1Z1[r, xi - 1]
            a = roll(V1Y2I[r], 127 - (16 * xi + 2), 1)
            s = V1Z1[r, xi] + V1Z1[r, xi - 2]
            s = s + roll(jnp.where(l127, a, c), 1, 1) + roll(jnp.where(l0, a, c), 127, 1)
            ins = jnp.where(r7, roll(V1M[r, xi, 0], 7, 0), roll(V1M[r, xi, 3], 1, 0))
            s = s + (V1Z2[r, x] + ins)
            V2Z[r, x] = E2Z[x] * c - C2 * s - sign(NZ1[xi - 1], 4 * r)
        for j in range(4):
            c = V1Y[r, j]
            s = roll(c, 1, 1) + roll(c, 127, 1) + (roll(c, 16, 1) + roll(c, 112, 1))
            zp = V1Y[r, j + 1] if j < 3 else roll(jnp.where(r0, V1Y2[r], V1Y[r, 0]), 7, 0)
            zm = V1Y[r, j - 1] if j > 0 else roll(jnp.where(r7, V1Y2[r], V1Y[r, 3]), 1, 0)
            s = s + (zp + zm)
            V2YI[r, j] = inner(E2Y[j] * c - C2 * s - sign(NY[j], 4 * r))
        return carry

    lax.fori_loop(0, 8, pass_b, 0)

    def pass_c(r, carry):
        for x in range(4):
            for j in range(4):
                c, s = around(
                    lambda xi, k: V2M[r, xi - 1, k], lambda xi: V2Z[r, xi - 2], V2YI[r, j], x + 2, j, None
                )
                cur[r, x, pl.ds(j, 8, stride=4), :] = E2M[x + 2, j] * c - C2 * s - V1M[r, x + 2, j]
        return carry

    lax.fori_loop(0, 8, pass_c, 0)

    @pl.when(core == 1)
    def _():
        for q in range(1, 64):
            plane_arrived(q)
        acc = jnp.zeros((8, 128), F32)
        for q in range(8):
            acc = acc + jnp.where(row + 8 * q == slot, mine, GP[8 * q : 8 * q + 8, :])
        S[1] = sum_rows(acc)
        for k in range(8):
            line_copy(k, 0).start()
        for k in range(1, 8):
            line_copy(k, 1).start()
        for k in range(1, 8):
            line_copy(k, 1).wait_recv()
        GL[pl.ds(gx, 1), :] = S[1, 0:1, :]

    @pl.when(core == 0)
    def _():
        for k in range(8):
            line_copy(k, 0).wait_recv()

    total = sum_rows(GL[...]) * (1.0 / NSITES)
    out = jnp.where(r0, total, jnp.where(row == 1, roll(total, 120, 1), roll(total, 112, 1)))
    mom[...] = out[:3, :8]
    for cp in halo:
        cp.wait_send()
    for k in range(1, 32):
        plane_copy(k).wait_send()

    @pl.when(core == 0)
    def _():
        plane_copy(0).wait_send()

    @pl.when(core == 1)
    def _():
        for k in range(8):
            line_copy(k, 0).wait_send()
        for k in range(1, 8):
            line_copy(k, 1).wait_send()


def write_out(mom, prev, cur, mom_out, prev_out, cur_out, sems):
    copies = [
        pltpu.make_async_copy(src, dst, sems.at[i])
        for i, (src, dst) in enumerate(((prev, prev_out), (cur, cur_out), (mom, mom_out)))
    ]
    for cp in copies:
        cp.start()
    for cp in copies:
        cp.wait()


def vm(*shape, dtype=F32):
    return pltpu.VMEM(shape + (8, 128), dtype)


def per_device(probe_bits, disorder_levels):
    dma = pltpu.SemaphoreType.DMA
    shapes = (
        jax.ShapeDtypeStruct((3, 8), F32),
        jax.ShapeDtypeStruct((8, 4, 32, 128), F32),
        jax.ShapeDtypeStruct((8, 4, 32, 128), F32),
    )
    held = pl.pallas_call(
        kernel,
        out_shape=shapes,
        in_specs=[pl.BlockSpec(memory_space=pltpu.HBM)] * 2,
        out_specs=(pl.BlockSpec(memory_space=pltpu.VMEM),) * 3,
        scratch_shapes=[
            pltpu.VMEM((2, 3, 10, 16, 128), I32),
            vm(8, 4, dtype=I32), vm(6, dtype=I32), vm(4, dtype=I32), vm(4, dtype=I32), vm(dtype=I32),
            vm(8, 4), vm(8, 4), vm(8, 4),
            vm(6), vm(6), vm(4), vm(4), vm(4),
            vm(4), vm(4), vm(4), vm(), vm(),
            vm(8, 8, 4), vm(8, 6), vm(8, 4), vm(8, 4), vm(8, 4), vm(8), vm(8),
            vm(8, 6, 4), vm(8, 4), vm(8, 4),
            vm(3), vm(2), pltpu.VMEM((64, 128), F32), vm(),
            dma((2,)), dma((26,)), dma((26,)), dma((32,)), dma((64,)), dma((16,)), dma((16,)),
        ],
        compiler_params=pltpu.CompilerParams(
            collective_id=0, has_side_effects=True, vmem_limit_bytes=24 * 1024 * 1024
        ),
    )(pltpu.with_memory_space_constraint(probe_bits, pltpu.HBM), pltpu.with_memory_space_constraint(disorder_levels, pltpu.HBM))
    return pl.pallas_call(
        write_out,
        out_shape=shapes,
        in_specs=[pl.BlockSpec(memory_space=pltpu.VMEM)] * 3,
        out_specs=(pl.BlockSpec(memory_space=pltpu.HBM),) * 3,
        scratch_shapes=[dma((3,))],
        compiler_params=pltpu.CompilerParams(vmem_limit_bytes=4 * 1024 * 1024),
    )(*held)


def solution(mesh):
    return jax.shard_map(
        per_device,
        mesh=mesh,
        in_specs=(P("gx", "gz", "gy"), P("gx", "gz", "gy")),
        out_specs=(P(), P(None, "gx", "gz", "gy"), P(None, "gx", "gz", "gy")),
        check_vma=False,
    )
```

```python
import jax
import jax.numpy as jnp
from jax import lax
from jax.experimental import pallas as pl
from jax.experimental.pallas import tpu as pltpu
from jax.sharding import PartitionSpec as P

F32 = jnp.float32
I32 = jnp.int32
MESH = pl.DeviceIdType.MESH
C2 = 2.0 / 8.4
NSITES = 32 * 512 * 512
LOCAL = 4 * 32 * 128

DIRS = sorted(
    [
        (dx, dy, dz)
        for dx in (-1, 0, 1)
        for dy in (-1, 0, 1)
        for dz in (-1, 0, 1)
        if (dx, dy, dz) != (0, 0, 0)
    ],
    key=lambda d: (-abs(d[2]), abs(d[0]) + abs(d[1])),
)


def srl(a, n):
    return lax.shift_right_logical(a, n if hasattr(n, "shape") and n.shape == a.shape else jnp.full(a.shape, n, I32))


def roll(a, n, axis):
    return pltpu.roll(a, n % a.shape[axis], axis)


def add_counts(s1, c1, s2, c2):
    h = s1 & s2
    z = c1 ^ c2
    return s1 ^ s2, z ^ h, (c1 & c2) | (h & z)


def nibbles(planes, word, shift):
    ones = 0x11111111
    p0, p1, p2 = planes
    return (
        (srl(p0, shift) & ones)
        | ((srl(p1, shift) & ones) << 1)
        | ((srl(p2, shift) & ones) << 2)
        | ((srl(word, shift) & ones) << 3)
    )


def kernel(
    bits_hbm, dis_hbm, mom, prev, cur,
    E, LAT, SG, NM, NZ1, NZ2, NY, NY2,
    EPM, EMM, E2M, EPZ1, EMZ1, EPZ2, EMZ2, E2Z, EPY, EMY, E2Y, EPY2, EMY2,
    V1M, V1Z1, V1Z2, V1Y, V1YI, V1Y2I, V1Y2, V2M, V2Z, V2YI, ACC, S, GP, GL,
    in_sem, hs, hr, ps, pr, ls, lr,
):
    gx, gy, gz = lax.axis_index("gx"), lax.axis_index("gy"), lax.axis_index("gz")
    yy, xhi = gz // 2, lax.rem(gz, 2)

    own_copies = [
        pltpu.make_async_copy(src, E.at[a, 1, 3:7, 0:8, :], in_sem.at[a])
        for a, src in enumerate((bits_hbm, dis_hbm))
    ]
    for cp in own_copies:
        cp.start()

    near_x = {d: lax.rem(gx + d + 8, 8) if d else gx for d in (-1, 0, 1)}
    near_y = {d: lax.rem(gy + d + 4, 4) if d else gy for d in (-1, 0, 1)}
    near_z = {d: lax.rem(gz + d + 16, 16) if d else gz for d in (-1, 0, 1)}

    def neighbour(d):
        return {"gx": near_x[d[0]], "gy": near_y[d[1]], "gz": near_z[d[2]]}

    core = lax.rem(gy, 2)
    pair = gy - core
    px = xhi * 2 + gy // 2
    place = yy * 4 + px
    line = [gx] + [lax.rem(gx + k, 8) for k in range(1, 8)]
    row_y = [yy * 2] + [lax.rem(yy + k, 8) * 2 for k in range(1, 8)]
    row_x = [px] + [lax.rem(px + k, 4) for k in range(1, 4)]
    row_h = [q // 2 for q in row_x]
    row_p = [(q - 2 * h) * 2 for q, h in zip(row_x, row_h)]

    def plane_peer(k, c):
        return {"gx": gx, "gy": row_p[k % 4] + c, "gz": row_y[k // 4] + row_h[k % 4]}

    def line_peer(k, c):
        return {"gx": line[k], "gy": pair + c, "gz": gz}

    barrier = pltpu.get_barrier_semaphore()

    def greet(device):
        pl.semaphore_signal(barrier, inc=1, device_id=device, device_id_type=MESH)

    for d in DIRS:
        greet(neighbour(d))
    for k in range(1, 8):
        greet(line_peer(k, 1))

    @pl.when(core == 0)
    def _():
        greet(line_peer(0, 1))

    @pl.when(core == 1)
    def _():
        for k in range(1, 32):
            greet(plane_peer(k, 1))
        for k in range(32):
            greet(plane_peer(k, 0))

    lane = lax.broadcasted_iota(I32, (8, 128), 1)
    row = lax.broadcasted_iota(I32, (8, 128), 0)
    l0, l127 = lane == 0, lane == 127
    r0, r7 = row == 0, row == 7

    for cp in own_copies:
        cp.wait()

    @pl.when(core == 0)
    def _():
        pl.semaphore_wait(barrier, 26 + 32)

    @pl.when(core == 1)
    def _():
        pl.semaphore_wait(barrier, 26 + 31 + 15)


    halo = []
    for i, (dx, dy, dz) in enumerate(DIRS):
        n = 3 - abs(dy) - abs(dz)
        if dx == 1:
            xs, xd = slice(7 - n, 7), slice(3 - n, 3)
        elif dx == -1:
            xs, xd = slice(3, 3 + n), slice(7, 7 + n)
        else:
            xs, xd = slice(3, 7), slice(3, 7)
        if dz == 1:
            ws, wd = slice(7, 8), slice(15, 16)
        elif dz == -1:
            ws, wd = slice(0, 1), slice(8, 9)
        else:
            ws, wd = slice(0, 8), slice(0, 8)
        cp = pltpu.make_async_remote_copy(
            src_ref=E.at[:, 1, xs, ws, :],
            dst_ref=E.at[:, 1 - dy, xd, wd, :],
            send_sem=hs.at[i],
            recv_sem=hr.at[i],
            device_id=neighbour((dx, dy, dz)),
            device_id_type=MESH,
        )
        cp.start()
        halo.append(cp)
    for cp, d in zip(halo, DIRS):
        if d[2] == 0:
            cp.wait_recv()

    def tile(a, t, xi, second):
        return E[a, t, xi + 1, (8 if second else 0) : (16 if second else 8), :]

    def pack_y(a, second):
        out = jnp.zeros((8, 128), I32)
        for xi in range(8):
            left, own, right = (tile(a, t, xi, second) for t in range(3))
            m1 = jnp.where(lane >= 64, left, own)
            m2 = jnp.where(lane >= 64, own, right)
            slot = lane - 16 * xi
            out = jnp.where((slot >= 0) & (slot < 8), roll(m1, 16 * xi - 125, 1), out)
            out = jnp.where((slot >= 8) & (slot < 16), roll(m2, 16 * xi + 8 - 126, 1), out)
        return out

    def up_down(main, second):
        up = roll(jnp.where(r0, second, main), 7, 0)
        down = roll(jnp.where(r7, second, main), 1, 0)
        return up, down

    def z_words(word, up, down):
        zp = (srl(word, 1) & 0x77777777) | (up << 3 & -0x77777778)
        zm = (word << 1 & -0x11111112) | (srl(down, 3) & 0x11111111)
        return zp, zm

    def sides(a, xi, second):
        left, own, right = (tile(a, t, xi, second) for t in range(3))
        return roll(jnp.where(l127, left, own), 1, 1), roll(jnp.where(l0, right, own), 127, 1)

    def energy(word, shift):
        return (srl(word, shift) & 255).astype(F32)

    def zshift(depth, unit):
        return jnp.where(row < 4, unit * (depth - 1), unit * (4 - depth))

    def weights(word, shift):
        lev = energy(word, shift)
        half = lev * (1.0 / 128.0)
        return half + (3.0 - 255.0 / 256.0 - 8.0), (3.0 + 255.0 / 256.0) - half

    def slope(word, shift):
        return energy(word, shift) * (C2 / 64.0) - (C2 * 255.0 / 128.0)

    def half_count(a, b, c):
        x = a ^ b
        return x ^ c, (a & b) | (c & x)

    for xi in range(8):
        dis = tile(1, 1, xi, False)
        for j in range(4):
            EPM[xi, j], EMM[xi, j] = weights(dis, 8 * j)
            if 1 <= xi <= 6:
                E2M[xi, j] = slope(dis, 8 * j)
        ym, yp = sides(0, xi, False)
        LAT[xi, 0], LAT[xi, 1] = half_count(tile(0, 1, xi + 1, False), tile(0, 1, xi - 1, False), yp)
        LAT[xi, 2] = ym
    yw, yd = pack_y(0, False), pack_y(1, False)
    for j in range(4):
        EPY[j], EMY[j] = weights(yd, 8 * j)
        E2Y[j] = slope(yd, 8 * j)
    for cp, d in zip(halo, DIRS):
        if d[2] != 0:
            cp.wait_recv()

    for xi in range(8):
        main, second = tile(0, 1, xi, False), tile(0, 1, xi, True)
        up, down = up_down(main, second)
        zp, zm = z_words(main, up, down)
        planes = add_counts(LAT[xi, 0], LAT[xi, 1], *half_count(LAT[xi, 2], zp, zm))
        for j in range(4):
            NM[xi, j] = nibbles(planes, main, j)
        if 1 <= xi <= 6:
            up, down = up_down(second, main)
            zp, zm = z_words(second, up, down)
            ym, yp = sides(0, xi, True)
            dis = tile(1, 1, xi, True)
            planes = add_counts(
                *half_count(tile(0, 1, xi + 1, True), tile(0, 1, xi - 1, True), yp),
                *half_count(ym, zp, zm),
            )
            NZ1[xi - 1] = nibbles(planes, second, zshift(1, 1))
            EPZ1[xi - 1], EMZ1[xi - 1] = weights(dis, zshift(1, 8))
            if 2 <= xi <= 5:
                E2Z[xi - 2] = slope(dis, zshift(1, 8))
                NZ2[xi - 2] = nibbles(planes, second, zshift(2, 1))
                EPZ2[xi - 2], EMZ2[xi - 2] = weights(dis, zshift(2, 8))

    yw2, yd2 = pack_y(0, True), pack_y(1, True)

    def y_planes(word, up, down):
        zp, zm = z_words(word, up, down)
        return add_counts(
            *half_count(roll(word, 1, 1), roll(word, 127, 1), roll(word, 16, 1)),
            *half_count(roll(word, 112, 1), zp, zm),
        )

    planes = y_planes(yw, *up_down(yw, yw2))
    for j in range(4):
        NY[j] = nibbles(planes, yw, j)
    planes = y_planes(yw2, *up_down(yw2, yw))
    NY2[...] = nibbles(planes, yw2, zshift(1, 1))
    EPY2[...], EMY2[...] = weights(yd2, zshift(1, 8))

    col = lane & 15

    def inner(y):
        return jnp.where(col == 1, roll(y, 119, 1), y)

    def top(word, sh):
        return word << jnp.full(word.shape, sh, I32)

    def first_order(word, ep, em, sh):
        t = top(word, sh)
        q = lax.shift_right_arithmetic(t, jnp.full(t.shape, 28, I32)).astype(F32)
        return jnp.where(t < 0, ep, em) - q

    def sign(word, sh):
        return jnp.where(top(word, sh) < 0, 1.0, -1.0).astype(F32)

    def around(get, edge, ins, xi, j):
        c = get(xi, j)
        a = roll(ins, 0 - (16 * xi + 2), 1)
        s = get(xi + 1, j) + get(xi - 1, j)
        s = s + (jnp.where(l0, a, roll(c, 1, 1)) + jnp.where(l127, a, roll(c, 127, 1)))
        zp = get(xi, j + 1) if j < 3 else roll(jnp.where(r0, edge(xi), get(xi, 0)), 7, 0)
        zm = get(xi, j - 1) if j > 0 else roll(jnp.where(r7, edge(xi), get(xi, 3)), 1, 0)
        return c, s + (zp + zm)

    def second_main(r, xi, j, sg):
        c, s = around(lambda x, k: V1M[r, x, k], lambda x: V1Z1[r, x - 1], V1YI[r, j], xi, j)
        return c, (E2M[xi, j] * c - C2 * s) * C2 - sg

    def pass_a1(r):
        sh = 28 - 4 * r
        for xi in range(8):
            for j in range(4):
                V1M[r, xi, j] = first_order(NM[xi, j], EPM[xi, j], EMM[xi, j], sh)
                if 2 <= xi <= 5:
                    SG[r, xi - 2, j] = sign(NM[xi, j], sh)
        for xi in range(6):
            V1Z1[r, xi] = first_order(NZ1[xi], EPZ1[xi], EMZ1[xi], sh)
        for xi in range(4):
            V1Z2[r, xi] = first_order(NZ2[xi], EPZ2[xi], EMZ2[xi], sh)
        for j in range(4):
            y = first_order(NY[j], EPY[j], EMY[j], sh)
            V1Y[r, j] = y
            V1YI[r, j] = inner(y)
        y = first_order(NY2[...], EPY2[...], EMY2[...], sh)
        V1Y2[r] = y
        V1Y2I[r] = inner(y)

    def pass_a2(r):
        a1 = jnp.zeros((8, 128), F32)
        a2 = jnp.zeros((8, 128), F32)
        a3 = jnp.zeros((8, 128), F32)
        for x in range(4):
            for j in range(4):
                sg = SG[r, x, j]
                v1, v2 = second_main(r, x + 2, j, sg)
                V2M[r, x + 1, j] = v2
                prev[r, x, pl.ds(j, 8, stride=4), :] = v2
                a1 = a1 + sg * v1
                a2 = a2 + v1 * v1
                a3 = a3 + v1 * v2
        a3 = (2.0 * C2) * a3 - C2 * a1
        a2 = (2.0 * C2 * C2) * a2 - float(LOCAL // 1024)
        for m, acc in enumerate((C2 * a1, a2, a3)):
            ACC[m, pl.ds(r, 1), :] = jnp.sum(acc, axis=0, keepdims=True)

    def probes(one, group):
        def body(g, carry):
            for i in range(group):
                one(g * group + i)
            return carry

        lax.fori_loop(0, 8 // group, body, 0)

    probes(pass_a1, 4)
    probes(pass_a2, 4)

    mine = jnp.zeros((8, 128), F32)
    for m in range(3):
        tot = jnp.sum(ACC[m], axis=1, keepdims=True)
        mine = mine + jnp.where(lane == row + 8 * m, jnp.broadcast_to(tot, (8, 128)), 0.0)

    def sum_rows(t):
        t = t + roll(t, 4, 0)
        t = t + roll(t, 2, 0)
        return t + roll(t, 1, 0)

    mine = sum_rows(mine)

    slot = place * 2 + core

    def plane_copy(k):
        return pltpu.make_async_remote_copy(
            src_ref=S.at[0, 0:1, :],
            dst_ref=GP.at[pl.ds(slot, 1), :],
            send_sem=ps.at[k],
            recv_sem=pr.at[(1 - core) * 32 + k],
            device_id=plane_peer(k, 1),
            device_id_type=MESH,
        )

    def line_copy(k, c):
        return pltpu.make_async_remote_copy(
            src_ref=S.at[1, 0:1, :],
            dst_ref=GL.at[pl.ds(gx, 1), :],
            send_sem=ls.at[c * 8 + k],
            recv_sem=lr.at[c * 8 + k],
            device_id=line_peer(k, c),
            device_id_type=MESH,
        )

    def plane_arrived(q):
        return pltpu.make_async_remote_copy(
            src_ref=S.at[0, 0:1, :],
            dst_ref=GP.at[0:1, :],
            send_sem=ps.at[0],
            recv_sem=pr.at[q],
            device_id=plane_peer(1, 1),
            device_id_type=MESH,
        ).wait_recv()

    S[0] = mine
    for k in range(1, 32):
        plane_copy(k).start()

    @pl.when(core == 0)
    def _():
        plane_copy(0).start()


    def pass_b(r):
        sh = 28 - 4 * r
        for xi, slot2 in ((1, 0), (6, 5)):
            for j in range(4):
                V2M[r, slot2, j] = second_main(r, xi, j, sign(NM[xi, j], sh))[1]
        for x in range(4):
            xi = x + 2
            c = V1Z1[r, xi - 1]
            a = roll(V1Y2I[r], 0 - (16 * xi + 2), 1)
            s = V1Z1[r, xi] + V1Z1[r, xi - 2]
            s = s + (jnp.where(l0, a, roll(c, 1, 1)) + jnp.where(l127, a, roll(c, 127, 1)))
            ins = jnp.where(r7, roll(V1M[r, xi, 0], 7, 0), roll(V1M[r, xi, 3], 1, 0))
            s = s + (V1Z2[r, x] + ins)
            V2Z[r, x] = (E2Z[x] * c - C2 * s) * C2 - sign(NZ1[xi - 1], sh)
        for j in range(4):
            c = V1Y[r, j]
            s = roll(c, 1, 1) + roll(c, 127, 1) + (roll(c, 16, 1) + roll(c, 112, 1))
            zp = V1Y[r, j + 1] if j < 3 else roll(jnp.where(r0, V1Y2[r], V1Y[r, 0]), 7, 0)
            zm = V1Y[r, j - 1] if j > 0 else roll(jnp.where(r7, V1Y2[r], V1Y[r, 3]), 1, 0)
            s = s + (zp + zm)
            V2YI[r, j] = inner((E2Y[j] * c - C2 * s) * C2 - sign(NY[j], sh))

    def pass_c(r):
        for x in range(4):
            for j in range(4):
                c, s = around(
                    lambda xi, k: V2M[r, xi - 1, k], lambda xi: V2Z[r, xi - 2], V2YI[r, j], x + 2, j
                )
                v3 = E2M[x + 2, j] * c - C2 * s - C2 * V1M[r, x + 2, j]
                cur[r, x, pl.ds(j, 8, stride=4), :] = v3

    probes(pass_b, 2)
    probes(pass_c, 4)

    @pl.when(core == 1)
    def _():
        for q in range(1, 64):
            plane_arrived(q)
        acc = jnp.zeros((8, 128), F32)
        for q in range(8):
            acc = acc + jnp.where(row + 8 * q == slot, mine, GP[8 * q : 8 * q + 8, :])
        S[1] = sum_rows(acc)
        for k in range(8):
            line_copy(k, 0).start()
        for k in range(1, 8):
            line_copy(k, 1).start()
        for k in range(1, 8):
            line_copy(k, 1).wait_recv()
        GL[pl.ds(gx, 1), :] = S[1, 0:1, :]

    @pl.when(core == 0)
    def _():
        for k in range(8):
            line_copy(k, 0).wait_recv()

    total = sum_rows(GL[...]) * (1.0 / NSITES)
    out = jnp.where(r0, total, jnp.where(row == 1, roll(total, 120, 1), roll(total, 112, 1)))
    mom[...] = out[:3, :8]
    for cp in halo:
        cp.wait_send()
    for k in range(1, 32):
        plane_copy(k).wait_send()

    @pl.when(core == 0)
    def _():
        plane_copy(0).wait_send()

    @pl.when(core == 1)
    def _():
        for k in range(8):
            line_copy(k, 0).wait_send()
        for k in range(1, 8):
            line_copy(k, 1).wait_send()


def write_out(mom, prev, cur, mom_out, prev_out, cur_out, sems):
    copies = [
        pltpu.make_async_copy(src, dst, sems.at[i])
        for i, (src, dst) in enumerate(((prev, prev_out), (cur, cur_out), (mom, mom_out)))
    ]
    for cp in copies:
        cp.start()
    for cp in copies:
        cp.wait()


def vm(*shape, dtype=F32):
    return pltpu.VMEM(shape + (8, 128), dtype)


def per_device(probe_bits, disorder_levels):
    dma = pltpu.SemaphoreType.DMA
    shapes = (
        jax.ShapeDtypeStruct((3, 8), F32),
        jax.ShapeDtypeStruct((8, 4, 32, 128), F32),
        jax.ShapeDtypeStruct((8, 4, 32, 128), F32),
    )
    held = pl.pallas_call(
        kernel,
        out_shape=shapes,
        in_specs=[pl.BlockSpec(memory_space=pltpu.HBM)] * 2,
        out_specs=(pl.BlockSpec(memory_space=pltpu.VMEM),) * 3,
        scratch_shapes=[
            pltpu.VMEM((2, 3, 10, 16, 128), I32),
            vm(8, 3, dtype=I32), vm(8, 4, 4), vm(8, 4, dtype=I32), vm(6, dtype=I32), vm(4, dtype=I32), vm(4, dtype=I32), vm(dtype=I32),
            vm(8, 4), vm(8, 4), vm(8, 4),
            vm(6), vm(6), vm(4), vm(4), vm(4),
            vm(4), vm(4), vm(4), vm(), vm(),
            vm(8, 8, 4), vm(8, 6), vm(8, 4), vm(8, 4), vm(8, 4), vm(8), vm(8),
            vm(8, 6, 4), vm(8, 4), vm(8, 4),
            vm(3), vm(2), pltpu.VMEM((64, 128), F32), vm(),
            dma((2,)), dma((26,)), dma((26,)), dma((32,)), dma((64,)), dma((16,)), dma((16,)),
        ],
        compiler_params=pltpu.CompilerParams(
            collective_id=0, has_side_effects=True, vmem_limit_bytes=24 * 1024 * 1024
        ),
    )(pltpu.with_memory_space_constraint(probe_bits, pltpu.HBM), pltpu.with_memory_space_constraint(disorder_levels, pltpu.HBM))
    return pl.pallas_call(
        write_out,
        out_shape=shapes,
        in_specs=[pl.BlockSpec(memory_space=pltpu.VMEM)] * 3,
        out_specs=(pl.BlockSpec(memory_space=pltpu.HBM),) * 3,
        scratch_shapes=[dma((3,))],
        compiler_params=pltpu.CompilerParams(vmem_limit_bytes=4 * 1024 * 1024),
    )(*held)


def solution(mesh):
    return jax.shard_map(
        per_device,
        mesh=mesh,
        in_specs=(P("gx", "gz", "gy"), P("gx", "gz", "gy")),
        out_specs=(P(), P(None, "gx", "gz", "gy"), P(None, "gx", "gz", "gy")),
        check_vma=False,
    )
```

```python
import jax
import jax.numpy as jnp
from jax import lax
from jax.experimental import pallas as pl
from jax.experimental.pallas import tpu as pltpu
from jax.sharding import PartitionSpec as P

F32 = jnp.float32
I32 = jnp.int32
MESH = pl.DeviceIdType.MESH
C2 = 2.0 / 8.4
NSITES = 32 * 512 * 512
LOCAL = 4 * 32 * 128

DIRS = sorted(
    [
        (dx, dy, dz)
        for dx in (-1, 0, 1)
        for dy in (-1, 0, 1)
        for dz in (-1, 0, 1)
        if (dx, dy, dz) != (0, 0, 0)
    ],
    key=lambda d: (-abs(d[2]), abs(d[0]) + abs(d[1])),
)


def srl(a, n):
    return lax.shift_right_logical(a, n if hasattr(n, "shape") and n.shape == a.shape else jnp.full(a.shape, n, I32))


def roll(a, n, axis):
    return pltpu.roll(a, n % a.shape[axis], axis)


def add_counts(s1, c1, s2, c2):
    h = s1 & s2
    z = c1 ^ c2
    return s1 ^ s2, z ^ h, (c1 & c2) | (h & z)


def nibbles(planes, word, shift):
    ones = 0x11111111
    p0, p1, p2 = planes
    return (
        (srl(p0, shift) & ones)
        | ((srl(p1, shift) & ones) << 1)
        | ((srl(p2, shift) & ones) << 2)
        | ((srl(word, shift) & ones) << 3)
    )


def kernel(
    bits_hbm, dis_hbm, mom, prev, cur,
    E, LAT, SG, NM, NZ1, NZ2, NY, NY2,
    EPM, EMM, E2M, EPZ1, EMZ1, EPZ2, EMZ2, E2Z, EPY, EMY, E2Y, EPY2, EMY2,
    V1M, V1Z1, V1Z2, V1Y, V1YI, V1Y2I, V1Y2, V2M, V2Z, V2YI, ACC, S, GP, GL,
    in_sem, hs, hr, ps, pr, ls, lr,
):
    gx, gy, gz = lax.axis_index("gx"), lax.axis_index("gy"), lax.axis_index("gz")
    yy, xhi = gz // 2, lax.rem(gz, 2)

    own_copies = [
        pltpu.make_async_copy(src, E.at[a, 1, 3:7, 0:8, :], in_sem.at[a])
        for a, src in enumerate((bits_hbm, dis_hbm))
    ]
    for cp in own_copies:
        cp.start()

    near_x = {d: lax.rem(gx + d + 8, 8) if d else gx for d in (-1, 0, 1)}
    near_y = {d: lax.rem(gy + d + 4, 4) if d else gy for d in (-1, 0, 1)}
    near_z = {d: lax.rem(gz + d + 16, 16) if d else gz for d in (-1, 0, 1)}

    def neighbour(d):
        return {"gx": near_x[d[0]], "gy": near_y[d[1]], "gz": near_z[d[2]]}

    core = lax.rem(gy, 2)
    pair = gy - core
    px = xhi * 2 + gy // 2
    place = yy * 4 + px
    line = [gx] + [lax.rem(gx + k, 8) for k in range(1, 8)]
    row_y = [yy * 2] + [lax.rem(yy + k, 8) * 2 for k in range(1, 8)]
    row_x = [px] + [lax.rem(px + k, 4) for k in range(1, 4)]
    row_h = [q // 2 for q in row_x]
    row_p = [(q - 2 * h) * 2 for q, h in zip(row_x, row_h)]

    def plane_peer(k, c):
        return {"gx": gx, "gy": row_p[k % 4] + c, "gz": row_y[k // 4] + row_h[k % 4]}

    def line_peer(k, c):
        return {"gx": line[k], "gy": pair + c, "gz": gz}

    barrier = pltpu.get_barrier_semaphore()

    def greet(device):
        pl.semaphore_signal(barrier, inc=1, device_id=device, device_id_type=MESH)

    for d in DIRS:
        greet(neighbour(d))
    for k in range(1, 8):
        greet(line_peer(k, 1))

    @pl.when(core == 0)
    def _():
        greet(line_peer(0, 1))

    @pl.when(core == 1)
    def _():
        for k in range(1, 32):
            greet(plane_peer(k, 1))
        for k in range(32):
            greet(plane_peer(k, 0))

    lane = lax.broadcasted_iota(I32, (8, 128), 1)
    row = lax.broadcasted_iota(I32, (8, 128), 0)
    l0, l127 = lane == 0, lane == 127
    r0, r7 = row == 0, row == 7

    for cp in own_copies:
        cp.wait()

    @pl.when(core == 0)
    def _():
        pl.semaphore_wait(barrier, 26 + 32)

    @pl.when(core == 1)
    def _():
        pl.semaphore_wait(barrier, 26 + 31 + 15)


    halo = []
    for i, (dx, dy, dz) in enumerate(DIRS):
        n = 3 - abs(dy) - abs(dz)
        if dx == 1:
            xs, xd = slice(7 - n, 7), slice(3 - n, 3)
        elif dx == -1:
            xs, xd = slice(3, 3 + n), slice(7, 7 + n)
        else:
            xs, xd = slice(3, 7), slice(3, 7)
        if dz == 1:
            ws, wd = slice(7, 8), slice(15, 16)
        elif dz == -1:
            ws, wd = slice(0, 1), slice(8, 9)
        else:
            ws, wd = slice(0, 8), slice(0, 8)
        cp = pltpu.make_async_remote_copy(
            src_ref=E.at[:, 1, xs, ws, :],
            dst_ref=E.at[:, 1 - dy, xd, wd, :],
            send_sem=hs.at[i],
            recv_sem=hr.at[i],
            device_id=neighbour((dx, dy, dz)),
            device_id_type=MESH,
        )
        cp.start()
        halo.append(cp)
    for cp, d in zip(halo, DIRS):
        if d[2] == 0:
            cp.wait_recv()

    def tile(a, t, xi, second):
        return E[a, t, xi + 1, (8 if second else 0) : (16 if second else 8), :]

    def pack_y(a, second):
        out = jnp.zeros((8, 128), I32)
        for xi in range(8):
            left, own, right = (tile(a, t, xi, second) for t in range(3))
            m1 = jnp.where(lane >= 64, left, own)
            m2 = jnp.where(lane >= 64, own, right)
            slot = lane - 16 * xi
            out = jnp.where((slot >= 0) & (slot < 8), roll(m1, 16 * xi - 125, 1), out)
            out = jnp.where((slot >= 8) & (slot < 16), roll(m2, 16 * xi + 8 - 126, 1), out)
        return out

    def up_down(main, second):
        up = roll(jnp.where(r0, second, main), 7, 0)
        down = roll(jnp.where(r7, second, main), 1, 0)
        return up, down

    def z_words(word, up, down):
        zp = (srl(word, 1) & 0x77777777) | (up << 3 & -0x77777778)
        zm = (word << 1 & -0x11111112) | (srl(down, 3) & 0x11111111)
        return zp, zm

    def sides(a, xi, second):
        left, own, right = (tile(a, t, xi, second) for t in range(3))
        return roll(jnp.where(l127, left, own), 1, 1), roll(jnp.where(l0, right, own), 127, 1)

    def energy(word, shift):
        return (srl(word, shift) & 255).astype(F32)

    def zshift(depth, unit):
        return jnp.where(row < 4, unit * (depth - 1), unit * (4 - depth))

    def weights(word, shift):
        lev = energy(word, shift)
        half = lev * (1.0 / 128.0)
        return half + (3.0 - 255.0 / 256.0 - 8.0), (3.0 + 255.0 / 256.0) - half

    def slope(word, shift):
        return energy(word, shift) * (C2 / 64.0) - (C2 * 255.0 / 128.0)

    def half_count(a, b, c):
        x = a ^ b
        return x ^ c, (a & b) | (c & x)

    for xi in range(8):
        dis = tile(1, 1, xi, False)
        for j in range(4):
            EPM[xi, j], EMM[xi, j] = weights(dis, 8 * j)
            if 1 <= xi <= 6:
                E2M[xi, j] = slope(dis, 8 * j)
        ym, yp = sides(0, xi, False)
        LAT[xi, 0], LAT[xi, 1] = half_count(tile(0, 1, xi + 1, False), tile(0, 1, xi - 1, False), yp)
        LAT[xi, 2] = ym
    yw, yd = pack_y(0, False), pack_y(1, False)
    for j in range(4):
        EPY[j], EMY[j] = weights(yd, 8 * j)
        E2Y[j] = slope(yd, 8 * j)
    for cp, d in zip(halo, DIRS):
        if d[2] != 0:
            cp.wait_recv()

    for xi in range(8):
        main, second = tile(0, 1, xi, False), tile(0, 1, xi, True)
        up, down = up_down(main, second)
        zp, zm = z_words(main, up, down)
        planes = add_counts(LAT[xi, 0], LAT[xi, 1], *half_count(LAT[xi, 2], zp, zm))
        for j in range(4):
            NM[xi, j] = nibbles(planes, main, j)
        if 1 <= xi <= 6:
            up, down = up_down(second, main)
            zp, zm = z_words(second, up, down)
            ym, yp = sides(0, xi, True)
            dis = tile(1, 1, xi, True)
            planes = add_counts(
                *half_count(tile(0, 1, xi + 1, True), tile(0, 1, xi - 1, True), yp),
                *half_count(ym, zp, zm),
            )
            NZ1[xi - 1] = nibbles(planes, second, zshift(1, 1))
            EPZ1[xi - 1], EMZ1[xi - 1] = weights(dis, zshift(1, 8))
            if 2 <= xi <= 5:
                E2Z[xi - 2] = slope(dis, zshift(1, 8))
                NZ2[xi - 2] = nibbles(planes, second, zshift(2, 1))
                EPZ2[xi - 2], EMZ2[xi - 2] = weights(dis, zshift(2, 8))

    yw2, yd2 = pack_y(0, True), pack_y(1, True)

    def y_planes(word, up, down):
        zp, zm = z_words(word, up, down)
        return add_counts(
            *half_count(roll(word, 1, 1), roll(word, 127, 1), roll(word, 16, 1)),
            *half_count(roll(word, 112, 1), zp, zm),
        )

    planes = y_planes(yw, *up_down(yw, yw2))
    for j in range(4):
        NY[j] = nibbles(planes, yw, j)
    planes = y_planes(yw2, *up_down(yw2, yw))
    NY2[...] = nibbles(planes, yw2, zshift(1, 1))
    EPY2[...], EMY2[...] = weights(yd2, zshift(1, 8))

    col = lane & 15

    def inner(y):
        return jnp.where(col == 1, roll(y, 119, 1), y)

    def top(word, sh):
        return word << jnp.full(word.shape, sh, I32)

    def first_order(word, ep, em, sh):
        t = top(word, sh)
        q = lax.shift_right_arithmetic(t, jnp.full(t.shape, 28, I32)).astype(F32)
        return jnp.where(t < 0, ep, em) - q

    def sign(word, sh):
        return jnp.where(top(word, sh) < 0, 1.0, -1.0).astype(F32)

    def around(get, edge, ins, xi, j):
        c = get(xi, j)
        a = roll(ins, 0 - (16 * xi + 2), 1)
        s = get(xi + 1, j) + get(xi - 1, j)
        s = s + (jnp.where(l0, a, roll(c, 1, 1)) + jnp.where(l127, a, roll(c, 127, 1)))
        zp = get(xi, j + 1) if j < 3 else roll(jnp.where(r0, edge(xi), get(xi, 0)), 7, 0)
        zm = get(xi, j - 1) if j > 0 else roll(jnp.where(r7, edge(xi), get(xi, 3)), 1, 0)
        return c, s + (zp + zm)

    def second_main(r, xi, j, sg):
        c, s = around(lambda x, k: V1M[r, x, k], lambda x: V1Z1[r, x - 1], V1YI[r, j], xi, j)
        return c, (E2M[xi, j] * c - C2 * s) * C2 - sg

    def pass_a1(r):
        sh = 28 - 4 * r
        for xi in range(8):
            for j in range(4):
                V1M[r, xi, j] = first_order(NM[xi, j], EPM[xi, j], EMM[xi, j], sh)
                if 2 <= xi <= 5:
                    SG[r, xi - 2, j] = sign(NM[xi, j], sh)
        for xi in range(6):
            V1Z1[r, xi] = first_order(NZ1[xi], EPZ1[xi], EMZ1[xi], sh)
        for xi in range(4):
            V1Z2[r, xi] = first_order(NZ2[xi], EPZ2[xi], EMZ2[xi], sh)
        for j in range(4):
            y = first_order(NY[j], EPY[j], EMY[j], sh)
            V1Y[r, j] = y
            V1YI[r, j] = inner(y)
        y = first_order(NY2[...], EPY2[...], EMY2[...], sh)
        V1Y2[r] = y
        V1Y2I[r] = inner(y)

    def pass_a2(r):
        a1 = jnp.zeros((8, 128), F32)
        a2 = jnp.zeros((8, 128), F32)
        a3 = jnp.zeros((8, 128), F32)
        for x in range(4):
            for j in range(4):
                sg = SG[r, x, j]
                v1, v2 = second_main(r, x + 2, j, sg)
                V2M[r, x + 1, j] = v2
                prev[r, x, pl.ds(j, 8, stride=4), :] = v2
                a1 = a1 + sg * v1
                a2 = a2 + v1 * v1
                a3 = a3 + v1 * v2
        a3 = (2.0 * C2) * a3 - C2 * a1
        a2 = (2.0 * C2 * C2) * a2 - float(LOCAL // 1024)
        for m, acc in enumerate((C2 * a1, a2, a3)):
            ACC[m, pl.ds(r, 1), :] = jnp.sum(acc, axis=0, keepdims=True)

    def probes(one, group):
        def body(g, carry):
            for i in range(group):
                one(g * group + i)
            return carry

        lax.fori_loop(0, 8 // group, body, 0)

    probes(pass_a1, 8)
    probes(pass_a2, 8)

    mine = jnp.zeros((8, 128), F32)
    for m in range(3):
        tot = jnp.sum(ACC[m], axis=1, keepdims=True)
        mine = mine + jnp.where(lane == row + 8 * m, jnp.broadcast_to(tot, (8, 128)), 0.0)

    def sum_rows(t):
        t = t + roll(t, 4, 0)
        t = t + roll(t, 2, 0)
        return t + roll(t, 1, 0)

    mine = sum_rows(mine)

    slot = place * 2 + core

    def plane_copy(k):
        return pltpu.make_async_remote_copy(
            src_ref=S.at[0, 0:1, :],
            dst_ref=GP.at[pl.ds(slot, 1), :],
            send_sem=ps.at[k],
            recv_sem=pr.at[(1 - core) * 32 + k],
            device_id=plane_peer(k, 1),
            device_id_type=MESH,
        )

    def line_copy(k, c):
        return pltpu.make_async_remote_copy(
            src_ref=S.at[1, 0:1, :],
            dst_ref=GL.at[pl.ds(gx, 1), :],
            send_sem=ls.at[c * 8 + k],
            recv_sem=lr.at[c * 8 + k],
            device_id=line_peer(k, c),
            device_id_type=MESH,
        )

    def plane_arrived(q):
        return pltpu.make_async_remote_copy(
            src_ref=S.at[0, 0:1, :],
            dst_ref=GP.at[0:1, :],
            send_sem=ps.at[0],
            recv_sem=pr.at[q],
            device_id=plane_peer(1, 1),
            device_id_type=MESH,
        ).wait_recv()

    S[0] = mine
    for k in range(1, 32):
        plane_copy(k).start()

    @pl.when(core == 0)
    def _():
        plane_copy(0).start()


    def pass_b(r):
        sh = 28 - 4 * r
        for xi, slot2 in ((1, 0), (6, 5)):
            for j in range(4):
                V2M[r, slot2, j] = second_main(r, xi, j, sign(NM[xi, j], sh))[1]
        for x in range(4):
            xi = x + 2
            c = V1Z1[r, xi - 1]
            a = roll(V1Y2I[r], 0 - (16 * xi + 2), 1)
            s = V1Z1[r, xi] + V1Z1[r, xi - 2]
            s = s + (jnp.where(l0, a, roll(c, 1, 1)) + jnp.where(l127, a, roll(c, 127, 1)))
            ins = jnp.where(r7, roll(V1M[r, xi, 0], 7, 0), roll(V1M[r, xi, 3], 1, 0))
            s = s + (V1Z2[r, x] + ins)
            V2Z[r, x] = (E2Z[x] * c - C2 * s) * C2 - sign(NZ1[xi - 1], sh)
        for j in range(4):
            c = V1Y[r, j]
            s = roll(c, 1, 1) + roll(c, 127, 1) + (roll(c, 16, 1) + roll(c, 112, 1))
            zp = V1Y[r, j + 1] if j < 3 else roll(jnp.where(r0, V1Y2[r], V1Y[r, 0]), 7, 0)
            zm = V1Y[r, j - 1] if j > 0 else roll(jnp.where(r7, V1Y2[r], V1Y[r, 3]), 1, 0)
            s = s + (zp + zm)
            V2YI[r, j] = inner((E2Y[j] * c - C2 * s) * C2 - sign(NY[j], sh))

    def pass_c(r):
        for x in range(4):
            for j in range(4):
                c, s = around(
                    lambda xi, k: V2M[r, xi - 1, k], lambda xi: V2Z[r, xi - 2], V2YI[r, j], x + 2, j
                )
                v3 = E2M[x + 2, j] * c - C2 * s - C2 * V1M[r, x + 2, j]
                cur[r, x, pl.ds(j, 8, stride=4), :] = v3

    probes(pass_b, 2)
    probes(pass_c, 4)

    @pl.when(core == 1)
    def _():
        for q in range(1, 64):
            plane_arrived(q)
        acc = jnp.zeros((8, 128), F32)
        for q in range(8):
            acc = acc + jnp.where(row + 8 * q == slot, mine, GP[8 * q : 8 * q + 8, :])
        S[1] = sum_rows(acc)
        for k in range(8):
            line_copy(k, 0).start()
        for k in range(1, 8):
            line_copy(k, 1).start()
        GL[pl.ds(gx, 1), :] = S[1, 0:1, :]

    for cp in halo:
        cp.wait_send()
    for k in range(1, 32):
        plane_copy(k).wait_send()

    @pl.when(core == 0)
    def _():
        plane_copy(0).wait_send()
        for k in range(8):
            line_copy(k, 0).wait_recv()

    @pl.when(core == 1)
    def _():
        for k in range(1, 8):
            line_copy(k, 1).wait_recv()

    total = sum_rows(GL[...]) * (1.0 / NSITES)
    out = jnp.where(r0, total, jnp.where(row == 1, roll(total, 120, 1), roll(total, 112, 1)))
    mom[...] = out[:3, :8]

    @pl.when(core == 1)
    def _():
        for k in range(8):
            line_copy(k, 0).wait_send()
        for k in range(1, 8):
            line_copy(k, 1).wait_send()


def write_out(mom, prev, cur, mom_out, prev_out, cur_out, sems):
    copies = [
        pltpu.make_async_copy(src, dst, sems.at[i])
        for i, (src, dst) in enumerate(((prev, prev_out), (cur, cur_out), (mom, mom_out)))
    ]
    for cp in copies:
        cp.start()
    for cp in copies:
        cp.wait()


def vm(*shape, dtype=F32):
    return pltpu.VMEM(shape + (8, 128), dtype)


def per_device(probe_bits, disorder_levels):
    dma = pltpu.SemaphoreType.DMA
    shapes = (
        jax.ShapeDtypeStruct((3, 8), F32),
        jax.ShapeDtypeStruct((8, 4, 32, 128), F32),
        jax.ShapeDtypeStruct((8, 4, 32, 128), F32),
    )
    held = pl.pallas_call(
        kernel,
        out_shape=shapes,
        in_specs=[pl.BlockSpec(memory_space=pltpu.HBM)] * 2,
        out_specs=(pl.BlockSpec(memory_space=pltpu.VMEM),) * 3,
        scratch_shapes=[
            pltpu.VMEM((2, 3, 10, 16, 128), I32),
            vm(8, 3, dtype=I32), vm(8, 4, 4), vm(8, 4, dtype=I32), vm(6, dtype=I32), vm(4, dtype=I32), vm(4, dtype=I32), vm(dtype=I32),
            vm(8, 4), vm(8, 4), vm(8, 4),
            vm(6), vm(6), vm(4), vm(4), vm(4),
            vm(4), vm(4), vm(4), vm(), vm(),
            vm(8, 8, 4), vm(8, 6), vm(8, 4), vm(8, 4), vm(8, 4), vm(8), vm(8),
            vm(8, 6, 4), vm(8, 4), vm(8, 4),
            vm(3), vm(2), pltpu.VMEM((64, 128), F32), vm(),
            dma((2,)), dma((26,)), dma((26,)), dma((32,)), dma((64,)), dma((16,)), dma((16,)),
        ],
        compiler_params=pltpu.CompilerParams(
            collective_id=0, has_side_effects=True, vmem_limit_bytes=24 * 1024 * 1024
        ),
    )(pltpu.with_memory_space_constraint(probe_bits, pltpu.HBM), pltpu.with_memory_space_constraint(disorder_levels, pltpu.HBM))
    return pl.pallas_call(
        write_out,
        out_shape=shapes,
        in_specs=[pl.BlockSpec(memory_space=pltpu.VMEM)] * 3,
        out_specs=(pl.BlockSpec(memory_space=pltpu.HBM),) * 3,
        scratch_shapes=[dma((3,))],
        compiler_params=pltpu.CompilerParams(vmem_limit_bytes=4 * 1024 * 1024),
    )(*held)


def solution(mesh):
    return jax.shard_map(
        per_device,
        mesh=mesh,
        in_specs=(P("gx", "gz", "gy"), P("gx", "gz", "gy")),
        out_specs=(P(), P(None, "gx", "gz", "gy"), P(None, "gx", "gz", "gy")),
        check_vma=False,
    )
```

```python
import jax
import jax.numpy as jnp
from jax import lax
from jax.experimental import pallas as pl
from jax.experimental.pallas import tpu as pltpu
from jax.sharding import PartitionSpec as P

F32 = jnp.float32
I32 = jnp.int32
MESH = pl.DeviceIdType.MESH
C2 = 2.0 / 8.4
NSITES = 32 * 512 * 512
LOCAL = 4 * 32 * 128

DIRS = sorted(
    [
        (dx, dy, dz)
        for dx in (-1, 0, 1)
        for dy in (-1, 0, 1)
        for dz in (-1, 0, 1)
        if (dx, dy, dz) != (0, 0, 0)
    ],
    key=lambda d: (-abs(d[2]), abs(d[0]) + abs(d[1])),
)


def srl(a, n):
    return lax.shift_right_logical(a, n if hasattr(n, "shape") and n.shape == a.shape else jnp.full(a.shape, n, I32))


def roll(a, n, axis):
    return pltpu.roll(a, n % a.shape[axis], axis)


def add_counts(s1, c1, s2, c2):
    h = s1 & s2
    z = c1 ^ c2
    return s1 ^ s2, z ^ h, (c1 & c2) | (h & z)


def nibbles(planes, word, shift):
    ones = 0x11111111
    p0, p1, p2 = planes
    return (
        (srl(p0, shift) & ones)
        | ((srl(p1, shift) & ones) << 1)
        | ((srl(p2, shift) & ones) << 2)
        | ((srl(word, shift) & ones) << 3)
    )


def kernel(
    bits_hbm, dis_hbm, mom, prev, cur,
    E, LAT, SG, NM, NZ1, NZ2, NY, NY2,
    EPM, EMM, E2M, EPZ1, EMZ1, EPZ2, EMZ2, E2Z, EPY, EMY, E2Y, EPY2, EMY2,
    V1M, V1Z1, V1Z2, V1Y, V1YI, V1Y2I, V1Y2, V2M, V2Z, V2YI, ACC, S, GP, GL,
    in_sem, hs, hr, ps, pr, ls, lr,
):
    gx, gy, gz = lax.axis_index("gx"), lax.axis_index("gy"), lax.axis_index("gz")
    yy, xhi = gz // 2, lax.rem(gz, 2)

    own_copies = [
        pltpu.make_async_copy(src, E.at[a, 1, 3:7, 0:8, :], in_sem.at[a])
        for a, src in enumerate((bits_hbm, dis_hbm))
    ]
    for cp in own_copies:
        cp.start()

    near_x = {d: lax.rem(gx + d + 8, 8) if d else gx for d in (-1, 0, 1)}
    near_y = {d: lax.rem(gy + d + 4, 4) if d else gy for d in (-1, 0, 1)}
    near_z = {d: lax.rem(gz + d + 16, 16) if d else gz for d in (-1, 0, 1)}

    def neighbour(d):
        return {"gx": near_x[d[0]], "gy": near_y[d[1]], "gz": near_z[d[2]]}

    core = lax.rem(gy, 2)
    pair = gy - core
    px = xhi * 2 + gy // 2
    place = yy * 4 + px
    line = [gx] + [lax.rem(gx + k, 8) for k in range(1, 8)]
    row_y = [yy * 2] + [lax.rem(yy + k, 8) * 2 for k in range(1, 8)]
    row_x = [px] + [lax.rem(px + k, 4) for k in range(1, 4)]
    row_h = [q // 2 for q in row_x]
    row_p = [(q - 2 * h) * 2 for q, h in zip(row_x, row_h)]

    def plane_peer(k, c):
        return {"gx": gx, "gy": row_p[k % 4] + c, "gz": row_y[k // 4] + row_h[k % 4]}

    def line_peer(k, c):
        return {"gx": line[k], "gy": pair + c, "gz": gz}

    barrier = pltpu.get_barrier_semaphore()

    def greet(device):
        pl.semaphore_signal(barrier, inc=1, device_id=device, device_id_type=MESH)

    for d in DIRS:
        greet(neighbour(d))
    for k in range(1, 8):
        greet(line_peer(k, 1))

    @pl.when(core == 0)
    def _():
        greet(line_peer(0, 1))

    @pl.when(core == 1)
    def _():
        for k in range(1, 32):
            greet(plane_peer(k, 1))
        for k in range(32):
            greet(plane_peer(k, 0))

    lane = lax.broadcasted_iota(I32, (8, 128), 1)
    row = lax.broadcasted_iota(I32, (8, 128), 0)
    l0, l127 = lane == 0, lane == 127
    r0, r7 = row == 0, row == 7

    for cp in own_copies:
        cp.wait()

    @pl.when(core == 0)
    def _():
        pl.semaphore_wait(barrier, 26 + 32)

    @pl.when(core == 1)
    def _():
        pl.semaphore_wait(barrier, 26 + 31 + 15)


    def halo_copy(i, d, lo, hi):
        dx, dy, dz = d
        if dx == 1:
            xs, xd = slice(7 - hi, 7 - lo), slice(3 - hi, 3 - lo)
        elif dx == -1:
            xs, xd = slice(3 + lo, 3 + hi), slice(7 + lo, 7 + hi)
        else:
            xs, xd = slice(3, 7), slice(3, 7)
        if dz == 1:
            ws, wd = slice(7, 8), slice(15, 16)
        elif dz == -1:
            ws, wd = slice(0, 1), slice(8, 9)
        else:
            ws, wd = slice(0, 8), slice(0, 8)
        return pltpu.make_async_remote_copy(
            src_ref=E.at[:, 1, xs, ws, :],
            dst_ref=E.at[:, 1 - dy, xd, wd, :],
            send_sem=hs.at[i],
            recv_sem=hr.at[i],
            device_id=neighbour(d),
            device_id_type=MESH,
        )

    first, rest = [], []
    for d in DIRS:
        depth = 2 - abs(d[1]) - abs(d[2])
        if d[0] == 0 or depth > 0:
            first.append((d, halo_copy(len(first), d, 0, depth)))
    for d in DIRS:
        depth = 2 - abs(d[1]) - abs(d[2])
        if d[0] != 0:
            rest.append((d, halo_copy(len(first) + len(rest), d, depth, depth + 1)))
    for d, cp in first + rest:
        cp.start()
    for d, cp in first:
        if d[2] == 0:
            cp.wait_recv()

    def tile(a, t, xi, second):
        return E[a, t, xi + 1, (8 if second else 0) : (16 if second else 8), :]

    def pack_y(a, second, span):
        out = jnp.zeros((8, 128), I32)
        for xi in span:
            left, own, right = (tile(a, t, xi, second) for t in range(3))
            m1 = jnp.where(lane >= 64, left, own)
            m2 = jnp.where(lane >= 64, own, right)
            slot = lane - 16 * xi
            out = jnp.where((slot >= 0) & (slot < 8), roll(m1, 16 * xi - 125, 1), out)
            out = jnp.where((slot >= 8) & (slot < 16), roll(m2, 16 * xi + 8 - 126, 1), out)
        return out

    def up_down(main, second):
        up = roll(jnp.where(r0, second, main), 7, 0)
        down = roll(jnp.where(r7, second, main), 1, 0)
        return up, down

    def z_words(word, up, down):
        zp = (srl(word, 1) & 0x77777777) | (up << 3 & -0x77777778)
        zm = (word << 1 & -0x11111112) | (srl(down, 3) & 0x11111111)
        return zp, zm

    def sides(a, xi, second):
        left, own, right = (tile(a, t, xi, second) for t in range(3))
        return roll(jnp.where(l127, left, own), 1, 1), roll(jnp.where(l0, right, own), 127, 1)

    def energy(word, shift):
        return (srl(word, shift) & 255).astype(F32)

    def zshift(depth, unit):
        return jnp.where(row < 4, unit * (depth - 1), unit * (4 - depth))

    def weights(word, shift):
        lev = energy(word, shift)
        half = lev * (1.0 / 128.0)
        return half + (3.0 - 255.0 / 256.0 - 8.0), (3.0 + 255.0 / 256.0) - half

    def slope(word, shift):
        return energy(word, shift) * (C2 / 64.0) - (C2 * 255.0 / 128.0)

    def half_count(a, b, c):
        x = a ^ b
        return x ^ c, (a & b) | (c & x)

    def main_near(xi):
        dis = tile(1, 1, xi, False)
        for j in range(4):
            EPM[xi, j], EMM[xi, j] = weights(dis, 8 * j)
        ym, yp = sides(0, xi, False)
        LAT[xi, 0], LAT[xi, 1] = half_count(tile(0, 1, xi + 1, False), tile(0, 1, xi - 1, False), yp)
        LAT[xi, 2] = ym

    def main_slope(xi):
        for j in range(4):
            E2M[xi, j] = slope(tile(1, 1, xi, False), 8 * j)

    def main_words(xi):
        main, second = tile(0, 1, xi, False), tile(0, 1, xi, True)
        zp, zm = z_words(main, *up_down(main, second))
        planes = add_counts(LAT[xi, 0], LAT[xi, 1], *half_count(LAT[xi, 2], zp, zm))
        for j in range(4):
            NM[xi, j] = nibbles(planes, main, j)

    def edge_words(xi, shallow, deep):
        main, second = tile(0, 1, xi, False), tile(0, 1, xi, True)
        zp, zm = z_words(second, *up_down(second, main))
        ym, yp = sides(0, xi, True)
        dis = tile(1, 1, xi, True)
        planes = add_counts(
            *half_count(tile(0, 1, xi + 1, True), tile(0, 1, xi - 1, True), yp),
            *half_count(ym, zp, zm),
        )
        if shallow:
            NZ1[xi - 1] = nibbles(planes, second, zshift(1, 1))
            EPZ1[xi - 1], EMZ1[xi - 1] = weights(dis, zshift(1, 8))
        if deep:
            E2Z[xi - 2] = slope(dis, zshift(1, 8))
            NZ2[xi - 2] = nibbles(planes, second, zshift(2, 1))
            EPZ2[xi - 2], EMZ2[xi - 2] = weights(dis, zshift(2, 8))

    def y_planes(word, up, down):
        zp, zm = z_words(word, up, down)
        return add_counts(
            *half_count(roll(word, 1, 1), roll(word, 127, 1), roll(word, 16, 1)),
            *half_count(roll(word, 112, 1), zp, zm),
        )

    def y_words(yw, yw2):
        planes = y_planes(yw, *up_down(yw, yw2))
        for j in range(4):
            NY[j] = nibbles(planes, yw, j)

    def y_weights(yd):
        for j in range(4):
            EPY[j], EMY[j] = weights(yd, 8 * j)

    for xi in range(1, 7):
        main_near(xi)
    for xi in range(2, 6):
        main_slope(xi)
    yw = pack_y(0, False, range(1, 7))
    y_weights(pack_y(1, False, range(1, 7)))

    for d, cp in first:
        if d[2] != 0:
            cp.wait_recv()

    for xi in range(1, 7):
        main_words(xi)
    for xi in range(2, 6):
        edge_words(xi, True, False)
    y_words(yw, pack_y(0, True, range(2, 6)))

    col = lane & 15

    def inner(y):
        return jnp.where(col == 1, roll(y, 119, 1), y)

    def top(word, sh):
        return word << jnp.full(word.shape, sh, I32)

    def first_order(word, ep, em, sh):
        t = top(word, sh)
        q = lax.shift_right_arithmetic(t, jnp.full(t.shape, 28, I32)).astype(F32)
        return jnp.where(t < 0, ep, em) - q

    def sign(word, sh):
        return jnp.where(top(word, sh) < 0, 1.0, -1.0).astype(F32)

    def around(get, edge, ins, xi, j):
        c = get(xi, j)
        a = roll(ins, 0 - (16 * xi + 2), 1)
        s = get(xi + 1, j) + get(xi - 1, j)
        s = s + (jnp.where(l0, a, roll(c, 1, 1)) + jnp.where(l127, a, roll(c, 127, 1)))
        zp = get(xi, j + 1) if j < 3 else roll(jnp.where(r0, edge(xi), get(xi, 0)), 7, 0)
        zm = get(xi, j - 1) if j > 0 else roll(jnp.where(r7, edge(xi), get(xi, 3)), 1, 0)
        return c, s + (zp + zm)

    def second_main(r, xi, j, sg):
        c, s = around(lambda x, k: V1M[r, x, k], lambda x: V1Z1[r, x - 1], V1YI[r, j], xi, j)
        return c, (E2M[xi, j] * c - C2 * s) * C2 - sg

    def main_first(r, xi, sh):
        for j in range(4):
            V1M[r, xi, j] = first_order(NM[xi, j], EPM[xi, j], EMM[xi, j], sh)

    def edge_first(r, xi, sh):
        V1Z1[r, xi - 1] = first_order(NZ1[xi - 1], EPZ1[xi - 1], EMZ1[xi - 1], sh)

    def y_first(r, sh):
        for j in range(4):
            y = first_order(NY[j], EPY[j], EMY[j], sh)
            V1Y[r, j] = y
            V1YI[r, j] = inner(y)

    def pass_a1(r):
        sh = 28 - 4 * r
        for xi in range(1, 7):
            main_first(r, xi, sh)
        for xi in range(2, 6):
            edge_first(r, xi, sh)
            for j in range(4):
                SG[r, xi - 2, j] = sign(NM[xi, j], sh)
        y_first(r, sh)

    def pass_a3(r):
        sh = 28 - 4 * r
        for xi in (0, 7):
            main_first(r, xi, sh)
        for xi in (1, 6):
            edge_first(r, xi, sh)
        for xi in range(4):
            V1Z2[r, xi] = first_order(NZ2[xi], EPZ2[xi], EMZ2[xi], sh)
        y_first(r, sh)
        y = first_order(NY2[...], EPY2[...], EMY2[...], sh)
        V1Y2[r] = y
        V1Y2I[r] = inner(y)

    def pass_a2(r):
        a1 = jnp.zeros((8, 128), F32)
        a2 = jnp.zeros((8, 128), F32)
        a3 = jnp.zeros((8, 128), F32)
        for x in range(4):
            for j in range(4):
                sg = SG[r, x, j]
                v1, v2 = second_main(r, x + 2, j, sg)
                V2M[r, x + 1, j] = v2
                prev[r, x, pl.ds(j, 8, stride=4), :] = v2
                a1 = a1 + sg * v1
                a2 = a2 + v1 * v1
                a3 = a3 + v1 * v2
        a3 = (2.0 * C2) * a3 - C2 * a1
        a2 = (2.0 * C2 * C2) * a2 - float(LOCAL // 1024)
        for m, acc in enumerate((C2 * a1, a2, a3)):
            ACC[m, pl.ds(r, 1), :] = jnp.sum(acc, axis=0, keepdims=True)

    def probes(one, group):
        def body(g, carry):
            for i in range(group):
                one(g * group + i)
            return carry

        lax.fori_loop(0, 8 // group, body, 0)

    probes(pass_a1, 8)
    probes(pass_a2, 8)

    mine = jnp.zeros((8, 128), F32)
    for m in range(3):
        tot = jnp.sum(ACC[m], axis=1, keepdims=True)
        mine = mine + jnp.where(lane == row + 8 * m, jnp.broadcast_to(tot, (8, 128)), 0.0)

    def sum_rows(t):
        t = t + roll(t, 4, 0)
        t = t + roll(t, 2, 0)
        return t + roll(t, 1, 0)

    mine = sum_rows(mine)

    slot = place * 2 + core

    def plane_copy(k):
        return pltpu.make_async_remote_copy(
            src_ref=S.at[0, 0:1, :],
            dst_ref=GP.at[pl.ds(slot, 1), :],
            send_sem=ps.at[k],
            recv_sem=pr.at[(1 - core) * 32 + k],
            device_id=plane_peer(k, 1),
            device_id_type=MESH,
        )

    def line_copy(k, c):
        return pltpu.make_async_remote_copy(
            src_ref=S.at[1, 0:1, :],
            dst_ref=GL.at[pl.ds(gx, 1), :],
            send_sem=ls.at[c * 8 + k],
            recv_sem=lr.at[c * 8 + k],
            device_id=line_peer(k, c),
            device_id_type=MESH,
        )

    def plane_arrived(q):
        return pltpu.make_async_remote_copy(
            src_ref=S.at[0, 0:1, :],
            dst_ref=GP.at[0:1, :],
            send_sem=ps.at[0],
            recv_sem=pr.at[q],
            device_id=plane_peer(1, 1),
            device_id_type=MESH,
        ).wait_recv()

    S[0] = mine
    for k in range(1, 32):
        plane_copy(k).start()

    @pl.when(core == 0)
    def _():
        plane_copy(0).start()


    for d, cp in rest:
        cp.wait_recv()
    for xi in (0, 7):
        main_near(xi)
        main_words(xi)
    for xi in (1, 6):
        main_slope(xi)
        edge_words(xi, True, False)
    for xi in range(2, 6):
        edge_words(xi, False, True)
    yw, yw2 = pack_y(0, False, range(8)), pack_y(0, True, range(8))
    yd, yd2 = pack_y(1, False, range(8)), pack_y(1, True, range(8))
    y_words(yw, yw2)
    y_weights(yd)
    for j in range(4):
        E2Y[j] = slope(yd, 8 * j)
    NY2[...] = nibbles(y_planes(yw2, *up_down(yw2, yw)), yw2, zshift(1, 1))
    EPY2[...], EMY2[...] = weights(yd2, zshift(1, 8))
    probes(pass_a3, 2)

    def pass_b(r):
        sh = 28 - 4 * r
        for xi, slot2 in ((1, 0), (6, 5)):
            for j in range(4):
                V2M[r, slot2, j] = second_main(r, xi, j, sign(NM[xi, j], sh))[1]
        for x in range(4):
            xi = x + 2
            c = V1Z1[r, xi - 1]
            a = roll(V1Y2I[r], 0 - (16 * xi + 2), 1)
            s = V1Z1[r, xi] + V1Z1[r, xi - 2]
            s = s + (jnp.where(l0, a, roll(c, 1, 1)) + jnp.where(l127, a, roll(c, 127, 1)))
            ins = jnp.where(r7, roll(V1M[r, xi, 0], 7, 0), roll(V1M[r, xi, 3], 1, 0))
            s = s + (V1Z2[r, x] + ins)
            V2Z[r, x] = (E2Z[x] * c - C2 * s) * C2 - sign(NZ1[xi - 1], sh)
        for j in range(4):
            c = V1Y[r, j]
            s = roll(c, 1, 1) + roll(c, 127, 1) + (roll(c, 16, 1) + roll(c, 112, 1))
            zp = V1Y[r, j + 1] if j < 3 else roll(jnp.where(r0, V1Y2[r], V1Y[r, 0]), 7, 0)
            zm = V1Y[r, j - 1] if j > 0 else roll(jnp.where(r7, V1Y2[r], V1Y[r, 3]), 1, 0)
            s = s + (zp + zm)
            V2YI[r, j] = inner((E2Y[j] * c - C2 * s) * C2 - sign(NY[j], sh))

    def pass_c(r):
        for x in range(4):
            for j in range(4):
                c, s = around(
                    lambda xi, k: V2M[r, xi - 1, k], lambda xi: V2Z[r, xi - 2], V2YI[r, j], x + 2, j
                )
                v3 = E2M[x + 2, j] * c - C2 * s - C2 * V1M[r, x + 2, j]
                cur[r, x, pl.ds(j, 8, stride=4), :] = v3

    probes(pass_b, 2)
    probes(pass_c, 4)

    @pl.when(core == 1)
    def _():
        for q in range(1, 64):
            plane_arrived(q)
        acc = jnp.zeros((8, 128), F32)
        for q in range(8):
            acc = acc + jnp.where(row + 8 * q == slot, mine, GP[8 * q : 8 * q + 8, :])
        S[1] = sum_rows(acc)
        for k in range(8):
            line_copy(k, 0).start()
        for k in range(1, 8):
            line_copy(k, 1).start()
        GL[pl.ds(gx, 1), :] = S[1, 0:1, :]

    for _, cp in first + rest:
        cp.wait_send()
    for k in range(1, 32):
        plane_copy(k).wait_send()

    @pl.when(core == 0)
    def _():
        plane_copy(0).wait_send()
        for k in range(8):
            line_copy(k, 0).wait_recv()

    @pl.when(core == 1)
    def _():
        for k in range(1, 8):
            line_copy(k, 1).wait_recv()

    total = sum_rows(GL[...]) * (1.0 / NSITES)
    out = jnp.where(r0, total, jnp.where(row == 1, roll(total, 120, 1), roll(total, 112, 1)))
    mom[...] = out[:3, :8]

    @pl.when(core == 1)
    def _():
        for k in range(8):
            line_copy(k, 0).wait_send()
        for k in range(1, 8):
            line_copy(k, 1).wait_send()


def write_out(mom, prev, cur, mom_out, prev_out, cur_out, sems):
    copies = [
        pltpu.make_async_copy(src, dst, sems.at[i])
        for i, (src, dst) in enumerate(((prev, prev_out), (cur, cur_out), (mom, mom_out)))
    ]
    for cp in copies:
        cp.start()
    for cp in copies:
        cp.wait()


def vm(*shape, dtype=F32):
    return pltpu.VMEM(shape + (8, 128), dtype)


def per_device(probe_bits, disorder_levels):
    dma = pltpu.SemaphoreType.DMA
    shapes = (
        jax.ShapeDtypeStruct((3, 8), F32),
        jax.ShapeDtypeStruct((8, 4, 32, 128), F32),
        jax.ShapeDtypeStruct((8, 4, 32, 128), F32),
    )
    held = pl.pallas_call(
        kernel,
        out_shape=shapes,
        in_specs=[pl.BlockSpec(memory_space=pltpu.HBM)] * 2,
        out_specs=(pl.BlockSpec(memory_space=pltpu.VMEM),) * 3,
        scratch_shapes=[
            pltpu.VMEM((2, 3, 10, 16, 128), I32),
            vm(8, 3, dtype=I32), vm(8, 4, 4), vm(8, 4, dtype=I32), vm(6, dtype=I32), vm(4, dtype=I32), vm(4, dtype=I32), vm(dtype=I32),
            vm(8, 4), vm(8, 4), vm(8, 4),
            vm(6), vm(6), vm(4), vm(4), vm(4),
            vm(4), vm(4), vm(4), vm(), vm(),
            vm(8, 8, 4), vm(8, 6), vm(8, 4), vm(8, 4), vm(8, 4), vm(8), vm(8),
            vm(8, 6, 4), vm(8, 4), vm(8, 4),
            vm(3), vm(2), pltpu.VMEM((64, 128), F32), vm(),
            dma((2,)), dma((38,)), dma((38,)), dma((32,)), dma((64,)), dma((16,)), dma((16,)),
        ],
        compiler_params=pltpu.CompilerParams(
            collective_id=0, has_side_effects=True, vmem_limit_bytes=24 * 1024 * 1024
        ),
    )(pltpu.with_memory_space_constraint(probe_bits, pltpu.HBM), pltpu.with_memory_space_constraint(disorder_levels, pltpu.HBM))
    return pl.pallas_call(
        write_out,
        out_shape=shapes,
        in_specs=[pl.BlockSpec(memory_space=pltpu.VMEM)] * 3,
        out_specs=(pl.BlockSpec(memory_space=pltpu.HBM),) * 3,
        scratch_shapes=[dma((3,))],
        compiler_params=pltpu.CompilerParams(vmem_limit_bytes=4 * 1024 * 1024),
    )(*held)


def solution(mesh):
    return jax.shard_map(
        per_device,
        mesh=mesh,
        in_specs=(P("gx", "gz", "gy"), P("gx", "gz", "gy")),
        out_specs=(P(), P(None, "gx", "gz", "gy"), P(None, "gx", "gz", "gy")),
        check_vma=False,
    )
```

```python
import jax
import jax.numpy as jnp
from jax import lax
from jax.experimental import pallas as pl
from jax.experimental.pallas import tpu as pltpu
from jax.sharding import PartitionSpec as P

F32 = jnp.float32
I32 = jnp.int32
MESH = pl.DeviceIdType.MESH
C2 = 2.0 / 8.4
NSITES = 32 * 512 * 512
LOCAL = 4 * 32 * 128

DIRS = sorted(
    [
        (dx, dy, dz)
        for dx in (-1, 0, 1)
        for dy in (-1, 0, 1)
        for dz in (-1, 0, 1)
        if (dx, dy, dz) != (0, 0, 0)
    ],
    key=lambda d: (-abs(d[2]), abs(d[0]) + abs(d[1])),
)


def srl(a, n):
    return lax.shift_right_logical(a, n if hasattr(n, "shape") and n.shape == a.shape else jnp.full(a.shape, n, I32))


def roll(a, n, axis):
    return pltpu.roll(a, n % a.shape[axis], axis)


def add_counts(s1, c1, s2, c2):
    h = s1 & s2
    z = c1 ^ c2
    return s1 ^ s2, z ^ h, (c1 & c2) | (h & z)


def nibbles(planes, word, shift):
    ones = 0x11111111
    p0, p1, p2 = planes
    return (
        (srl(p0, shift) & ones)
        | ((srl(p1, shift) & ones) << 1)
        | ((srl(p2, shift) & ones) << 2)
        | ((srl(word, shift) & ones) << 3)
    )


def kernel(
    bits_hbm, dis_hbm, mom, prev, cur,
    E, LAT, NM, NZ1, NZ2, NY, NY2,
    EPM, EMM, E2M, EPZ1, EMZ1, EPZ2, EMZ2, E2Z, EPY, EMY, E2Y, EPY2, EMY2,
    V1M, V1Z1, V1Z2, V1Y, V1YI, V1Y2I, V1Y2, V2M, V2Z, V2YI, ACC, S, GP, GL,
    in_sem, hs, hr, ps, pr, ls, lr,
):
    gx, gy, gz = lax.axis_index("gx"), lax.axis_index("gy"), lax.axis_index("gz")
    yy, xhi = gz // 2, lax.rem(gz, 2)

    own_copies = [
        pltpu.make_async_copy(src, E.at[a, 1, 3:7, 0:8, :], in_sem.at[a])
        for a, src in enumerate((bits_hbm, dis_hbm))
    ]
    for cp in own_copies:
        cp.start()

    near_x = {d: lax.rem(gx + d + 8, 8) if d else gx for d in (-1, 0, 1)}
    near_y = {d: lax.rem(gy + d + 4, 4) if d else gy for d in (-1, 0, 1)}
    near_z = {d: lax.rem(gz + d + 16, 16) if d else gz for d in (-1, 0, 1)}

    def neighbour(d):
        return {"gx": near_x[d[0]], "gy": near_y[d[1]], "gz": near_z[d[2]]}

    core = lax.rem(gy, 2)
    pair = gy - core
    px = xhi * 2 + gy // 2
    place = yy * 4 + px
    line = [gx] + [lax.rem(gx + k, 8) for k in range(1, 8)]
    row_y = [yy * 2] + [lax.rem(yy + k, 8) * 2 for k in range(1, 8)]
    row_x = [px] + [lax.rem(px + k, 4) for k in range(1, 4)]
    row_h = [q // 2 for q in row_x]
    row_p = [(q - 2 * h) * 2 for q, h in zip(row_x, row_h)]

    def plane_peer(k, c):
        return {"gx": gx, "gy": row_p[k % 4] + c, "gz": row_y[k // 4] + row_h[k % 4]}

    def line_peer(k, c):
        return {"gx": line[k], "gy": pair + c, "gz": gz}

    barrier = pltpu.get_barrier_semaphore()

    def greet(device):
        pl.semaphore_signal(barrier, inc=1, device_id=device, device_id_type=MESH)

    for d in DIRS:
        greet(neighbour(d))
    for k in range(1, 8):
        greet(line_peer(k, 1))

    @pl.when(core == 0)
    def _():
        greet(line_peer(0, 1))

    @pl.when(core == 1)
    def _():
        for k in range(1, 32):
            greet(plane_peer(k, 1))
        for k in range(32):
            greet(plane_peer(k, 0))

    lane = lax.broadcasted_iota(I32, (8, 128), 1)
    row = lax.broadcasted_iota(I32, (8, 128), 0)
    l0, l127 = lane == 0, lane == 127
    r0, r7 = row == 0, row == 7

    for cp in own_copies:
        cp.wait()

    @pl.when(core == 0)
    def _():
        pl.semaphore_wait(barrier, 26 + 32)

    @pl.when(core == 1)
    def _():
        pl.semaphore_wait(barrier, 26 + 31 + 15)


    def halo_copy(i, d, lo, hi):
        dx, dy, dz = d
        if dx == 1:
            xs, xd = slice(7 - hi, 7 - lo), slice(3 - hi, 3 - lo)
        elif dx == -1:
            xs, xd = slice(3 + lo, 3 + hi), slice(7 + lo, 7 + hi)
        else:
            xs, xd = slice(3, 7), slice(3, 7)
        if dz == 1:
            ws, wd = slice(7, 8), slice(15, 16)
        elif dz == -1:
            ws, wd = slice(0, 1), slice(8, 9)
        else:
            ws, wd = slice(0, 8), slice(0, 8)
        return pltpu.make_async_remote_copy(
            src_ref=E.at[:, 1, xs, ws, :],
            dst_ref=E.at[:, 1 - dy, xd, wd, :],
            send_sem=hs.at[i],
            recv_sem=hr.at[i],
            device_id=neighbour(d),
            device_id_type=MESH,
        )

    first, rest = [], []
    for d in DIRS:
        depth = 2 - abs(d[1]) - abs(d[2])
        if d[0] == 0 or depth > 0:
            first.append((d, halo_copy(len(first), d, 0, depth)))
    for d in DIRS:
        depth = 2 - abs(d[1]) - abs(d[2])
        if d[0] != 0:
            rest.append((d, halo_copy(len(first) + len(rest), d, depth, depth + 1)))
    for d, cp in first + rest:
        cp.start()
    for d, cp in first:
        if d[2] == 0:
            cp.wait_recv()

    def tile(a, t, xi, second):
        return E[a, t, xi + 1, (8 if second else 0) : (16 if second else 8), :]

    def pack_y(a, second, span):
        out = jnp.zeros((8, 128), I32)
        for xi in span:
            left, own, right = (tile(a, t, xi, second) for t in range(3))
            m1 = jnp.where(lane >= 64, left, own)
            m2 = jnp.where(lane >= 64, own, right)
            slot = lane - 16 * xi
            out = jnp.where((slot >= 0) & (slot < 8), roll(m1, 16 * xi - 125, 1), out)
            out = jnp.where((slot >= 8) & (slot < 16), roll(m2, 16 * xi + 8 - 126, 1), out)
        return out

    def up_down(main, second):
        up = roll(jnp.where(r0, second, main), 7, 0)
        down = roll(jnp.where(r7, second, main), 1, 0)
        return up, down

    def z_words(word, up, down):
        zp = (srl(word, 1) & 0x77777777) | (up << 3 & -0x77777778)
        zm = (word << 1 & -0x11111112) | (srl(down, 3) & 0x11111111)
        return zp, zm

    def sides(a, xi, second):
        left, own, right = (tile(a, t, xi, second) for t in range(3))
        return roll(jnp.where(l127, left, own), 1, 1), roll(jnp.where(l0, right, own), 127, 1)

    def energy(word, shift):
        return (srl(word, shift) & 255).astype(F32)

    def zshift(depth, unit):
        return jnp.where(row < 4, unit * (depth - 1), unit * (4 - depth))

    def weights(word, shift):
        lev = energy(word, shift)
        half = lev * (1.0 / 128.0)
        return half + (3.0 - 255.0 / 256.0 - 8.0), (3.0 + 255.0 / 256.0) - half

    def slope(word, shift):
        return energy(word, shift) * (C2 / 64.0) - (C2 * 255.0 / 128.0)

    def half_count(a, b, c):
        x = a ^ b
        return x ^ c, (a & b) | (c & x)

    def main_near(xi):
        dis = tile(1, 1, xi, False)
        for j in range(4):
            EPM[xi, j], EMM[xi, j] = weights(dis, 8 * j)
        ym, yp = sides(0, xi, False)
        LAT[xi, 0], LAT[xi, 1] = half_count(tile(0, 1, xi + 1, False), tile(0, 1, xi - 1, False), yp)
        LAT[xi, 2] = ym

    def main_slope(xi):
        for j in range(4):
            E2M[xi, j] = slope(tile(1, 1, xi, False), 8 * j)

    def main_words(xi):
        main, second = tile(0, 1, xi, False), tile(0, 1, xi, True)
        zp, zm = z_words(main, *up_down(main, second))
        planes = add_counts(LAT[xi, 0], LAT[xi, 1], *half_count(LAT[xi, 2], zp, zm))
        for j in range(4):
            NM[xi, j] = nibbles(planes, main, j)

    def edge_words(xi, shallow, deep):
        main, second = tile(0, 1, xi, False), tile(0, 1, xi, True)
        zp, zm = z_words(second, *up_down(second, main))
        ym, yp = sides(0, xi, True)
        dis = tile(1, 1, xi, True)
        planes = add_counts(
            *half_count(tile(0, 1, xi + 1, True), tile(0, 1, xi - 1, True), yp),
            *half_count(ym, zp, zm),
        )
        if shallow:
            NZ1[xi - 1] = nibbles(planes, second, zshift(1, 1))
            EPZ1[xi - 1], EMZ1[xi - 1] = weights(dis, zshift(1, 8))
        if deep:
            E2Z[xi - 2] = slope(dis, zshift(1, 8))
            NZ2[xi - 2] = nibbles(planes, second, zshift(2, 1))
            EPZ2[xi - 2], EMZ2[xi - 2] = weights(dis, zshift(2, 8))

    def y_planes(word, up, down):
        zp, zm = z_words(word, up, down)
        return add_counts(
            *half_count(roll(word, 1, 1), roll(word, 127, 1), roll(word, 16, 1)),
            *half_count(roll(word, 112, 1), zp, zm),
        )

    def y_words(yw, yw2):
        planes = y_planes(yw, *up_down(yw, yw2))
        for j in range(4):
            NY[j] = nibbles(planes, yw, j)

    def y_weights(yd):
        for j in range(4):
            EPY[j], EMY[j] = weights(yd, 8 * j)

    for xi in range(1, 7):
        main_near(xi)
    for xi in range(2, 6):
        main_slope(xi)
    yw = pack_y(0, False, range(1, 7))
    y_weights(pack_y(1, False, range(1, 7)))

    for d, cp in first:
        if d[2] != 0:
            cp.wait_recv()

    for xi in range(1, 7):
        main_words(xi)
    for xi in range(2, 6):
        edge_words(xi, True, False)
    y_words(yw, pack_y(0, True, range(2, 6)))

    col = lane & 15

    def inner(y):
        return jnp.where(col == 1, roll(y, 119, 1), y)

    def top(word, sh):
        return word << jnp.full(word.shape, sh, I32)

    def first_order(word, ep, em, sh):
        t = top(word, sh)
        q = lax.shift_right_arithmetic(t, jnp.full(t.shape, 28, I32)).astype(F32)
        return jnp.where(t < 0, ep, em) - q

    def sign(word, sh):
        return jnp.where(top(word, sh) < 0, 1.0, -1.0).astype(F32)

    def around(get, edge, ins, xi, j):
        c = get(xi, j)
        a = roll(ins, 0 - (16 * xi + 2), 1)
        s = get(xi + 1, j) + get(xi - 1, j)
        s = s + (jnp.where(l0, a, roll(c, 1, 1)) + jnp.where(l127, a, roll(c, 127, 1)))
        zp = get(xi, j + 1) if j < 3 else roll(jnp.where(r0, edge(xi), get(xi, 0)), 7, 0)
        zm = get(xi, j - 1) if j > 0 else roll(jnp.where(r7, edge(xi), get(xi, 3)), 1, 0)
        return c, s + (zp + zm)

    def second_main(r, xi, j, sg):
        c, s = around(lambda x, k: V1M[r, x, k], lambda x: V1Z1[r, x - 1], V1YI[r, j], xi, j)
        return c, (E2M[xi, j] * c - C2 * s) * C2 - sg

    def main_first(r, xi, sh):
        for j in range(4):
            V1M[r, xi, j] = first_order(NM[xi, j], EPM[xi, j], EMM[xi, j], sh)

    def edge_first(r, xi, sh):
        V1Z1[r, xi - 1] = first_order(NZ1[xi - 1], EPZ1[xi - 1], EMZ1[xi - 1], sh)

    def y_first(r, sh):
        for j in range(4):
            y = first_order(NY[j], EPY[j], EMY[j], sh)
            V1Y[r, j] = y
            V1YI[r, j] = inner(y)

    def pass_a1(r):
        sh = 28 - 4 * r
        for xi in range(2, 7):
            main_first(r, xi, sh)
        for xi in range(2, 6):
            edge_first(r, xi, sh)
        y_first(r, sh)

    def pass_a3(r):
        sh = 28 - 4 * r
        for xi in (0, 1, 7):
            main_first(r, xi, sh)
        for xi in (1, 6):
            edge_first(r, xi, sh)
        for xi in range(4):
            V1Z2[r, xi] = first_order(NZ2[xi], EPZ2[xi], EMZ2[xi], sh)
        y_first(r, sh)
        y = first_order(NY2[...], EPY2[...], EMY2[...], sh)
        V1Y2[r] = y
        V1Y2I[r] = inner(y)

    def moments_of(r):
        sh = 28 - 4 * r
        own = jnp.zeros((8, 128), F32)
        square = jnp.zeros((8, 128), F32)
        onsite = jnp.zeros((8, 128), F32)
        bonds = jnp.zeros((8, 128), F32)
        for xi in range(2, 6):
            for j in range(4):
                c = V1M[r, xi, j]
                side = roll(V1YI[r, j], 0 - (16 * xi + 2), 1)
                above = V1M[r, xi, j + 1] if j < 3 else roll(jnp.where(r0, V1Z1[r, xi - 1], V1M[r, xi, 0]), 7, 0)
                ahead = V1M[r, xi + 1, j] + jnp.where(l127, side, roll(c, 127, 1)) + above
                c2 = c * c
                own = own + jnp.where(top(NM[xi, j], sh) < 0, c, 0.0 - c)
                square = square + c2
                onsite = onsite + E2M[xi, j] * c2
                bonds = bonds + c * ahead
        m3 = (2.0 * C2 * C2) * (onsite - (2.0 * C2) * bonds) - (3.0 * C2) * own
        m2 = (2.0 * C2 * C2) * square - float(LOCAL // 1024)
        for m, acc in enumerate((C2 * own, m2, m3)):
            ACC[m, pl.ds(r, 1), :] = jnp.sum(acc, axis=0, keepdims=True)

    def pass_a2(r):
        sh = 28 - 4 * r
        for x in range(4):
            for j in range(4):
                v2 = second_main(r, x + 2, j, sign(NM[x + 2, j], sh))[1]
                V2M[r, x + 1, j] = v2
                prev[r, x, pl.ds(j, 8, stride=4), :] = v2

    def probes(one, group):
        def body(g, carry):
            for i in range(group):
                one(g * group + i)
            return carry

        lax.fori_loop(0, 8 // group, body, 0)

    probes(pass_a1, 8)
    probes(moments_of, 8)

    mine = jnp.zeros((8, 128), F32)
    for m in range(3):
        tot = jnp.sum(ACC[m], axis=1, keepdims=True)
        mine = mine + jnp.where(lane == row + 8 * m, jnp.broadcast_to(tot, (8, 128)), 0.0)

    def sum_rows(t):
        t = t + roll(t, 4, 0)
        t = t + roll(t, 2, 0)
        return t + roll(t, 1, 0)

    mine = sum_rows(mine)

    slot = place * 2 + core

    def plane_copy(k):
        return pltpu.make_async_remote_copy(
            src_ref=S.at[0, 0:1, :],
            dst_ref=GP.at[pl.ds(slot, 1), :],
            send_sem=ps.at[k],
            recv_sem=pr.at[(1 - core) * 32 + k],
            device_id=plane_peer(k, 1),
            device_id_type=MESH,
        )

    def line_copy(k, c):
        return pltpu.make_async_remote_copy(
            src_ref=S.at[1, 0:1, :],
            dst_ref=GL.at[pl.ds(gx, 1), :],
            send_sem=ls.at[c * 8 + k],
            recv_sem=lr.at[c * 8 + k],
            device_id=line_peer(k, c),
            device_id_type=MESH,
        )

    def plane_arrived(q):
        return pltpu.make_async_remote_copy(
            src_ref=S.at[0, 0:1, :],
            dst_ref=GP.at[0:1, :],
            send_sem=ps.at[0],
            recv_sem=pr.at[q],
            device_id=plane_peer(1, 1),
            device_id_type=MESH,
        ).wait_recv()

    S[0] = mine
    for k in range(1, 32):
        plane_copy(k).start()

    @pl.when(core == 0)
    def _():
        plane_copy(0).start()


    for d, cp in rest:
        cp.wait_recv()
    for xi in (0, 7):
        main_near(xi)
        main_words(xi)
    for xi in (1, 6):
        main_slope(xi)
        edge_words(xi, True, False)
    for xi in range(2, 6):
        edge_words(xi, False, True)
    yw, yw2 = pack_y(0, False, range(8)), pack_y(0, True, range(8))
    yd, yd2 = pack_y(1, False, range(8)), pack_y(1, True, range(8))
    y_words(yw, yw2)
    y_weights(yd)
    for j in range(4):
        E2Y[j] = slope(yd, 8 * j)
    NY2[...] = nibbles(y_planes(yw2, *up_down(yw2, yw)), yw2, zshift(1, 1))
    EPY2[...], EMY2[...] = weights(yd2, zshift(1, 8))
    probes(pass_a3, 2)
    probes(pass_a2, 4)

    def pass_b(r):
        sh = 28 - 4 * r
        for xi, slot2 in ((1, 0), (6, 5)):
            for j in range(4):
                V2M[r, slot2, j] = second_main(r, xi, j, sign(NM[xi, j], sh))[1]
        for x in range(4):
            xi = x + 2
            c = V1Z1[r, xi - 1]
            a = roll(V1Y2I[r], 0 - (16 * xi + 2), 1)
            s = V1Z1[r, xi] + V1Z1[r, xi - 2]
            s = s + (jnp.where(l0, a, roll(c, 1, 1)) + jnp.where(l127, a, roll(c, 127, 1)))
            ins = jnp.where(r7, roll(V1M[r, xi, 0], 7, 0), roll(V1M[r, xi, 3], 1, 0))
            s = s + (V1Z2[r, x] + ins)
            V2Z[r, x] = (E2Z[x] * c - C2 * s) * C2 - sign(NZ1[xi - 1], sh)
        for j in range(4):
            c = V1Y[r, j]
            s = roll(c, 1, 1) + roll(c, 127, 1) + (roll(c, 16, 1) + roll(c, 112, 1))
            zp = V1Y[r, j + 1] if j < 3 else roll(jnp.where(r0, V1Y2[r], V1Y[r, 0]), 7, 0)
            zm = V1Y[r, j - 1] if j > 0 else roll(jnp.where(r7, V1Y2[r], V1Y[r, 3]), 1, 0)
            s = s + (zp + zm)
            V2YI[r, j] = inner((E2Y[j] * c - C2 * s) * C2 - sign(NY[j], sh))

    def pass_c(r):
        for x in range(4):
            for j in range(4):
                c, s = around(
                    lambda xi, k: V2M[r, xi - 1, k], lambda xi: V2Z[r, xi - 2], V2YI[r, j], x + 2, j
                )
                v3 = E2M[x + 2, j] * c - C2 * s - C2 * V1M[r, x + 2, j]
                cur[r, x, pl.ds(j, 8, stride=4), :] = v3

    probes(pass_b, 2)
    probes(pass_c, 4)

    @pl.when(core == 1)
    def _():
        for q in range(1, 64):
            plane_arrived(q)
        acc = jnp.zeros((8, 128), F32)
        for q in range(8):
            acc = acc + jnp.where(row + 8 * q == slot, mine, GP[8 * q : 8 * q + 8, :])
        S[1] = sum_rows(acc)
        for k in range(8):
            line_copy(k, 0).start()
        for k in range(1, 8):
            line_copy(k, 1).start()
        GL[pl.ds(gx, 1), :] = S[1, 0:1, :]

    for _, cp in first + rest:
        cp.wait_send()
    for k in range(1, 32):
        plane_copy(k).wait_send()

    @pl.when(core == 0)
    def _():
        plane_copy(0).wait_send()
        for k in range(8):
            line_copy(k, 0).wait_recv()

    @pl.when(core == 1)
    def _():
        for k in range(1, 8):
            line_copy(k, 1).wait_recv()

    total = sum_rows(GL[...]) * (1.0 / NSITES)
    out = jnp.where(r0, total, jnp.where(row == 1, roll(total, 120, 1), roll(total, 112, 1)))
    mom[...] = out[:3, :8]

    @pl.when(core == 1)
    def _():
        for k in range(8):
            line_copy(k, 0).wait_send()
        for k in range(1, 8):
            line_copy(k, 1).wait_send()


def write_out(mom, prev, cur, mom_out, prev_out, cur_out, sems):
    copies = [
        pltpu.make_async_copy(src, dst, sems.at[i])
        for i, (src, dst) in enumerate(((prev, prev_out), (cur, cur_out), (mom, mom_out)))
    ]
    for cp in copies:
        cp.start()
    for cp in copies:
        cp.wait()


def vm(*shape, dtype=F32):
    return pltpu.VMEM(shape + (8, 128), dtype)


def per_device(probe_bits, disorder_levels):
    dma = pltpu.SemaphoreType.DMA
    shapes = (
        jax.ShapeDtypeStruct((3, 8), F32),
        jax.ShapeDtypeStruct((8, 4, 32, 128), F32),
        jax.ShapeDtypeStruct((8, 4, 32, 128), F32),
    )
    held = pl.pallas_call(
        kernel,
        out_shape=shapes,
        in_specs=[pl.BlockSpec(memory_space=pltpu.HBM)] * 2,
        out_specs=(pl.BlockSpec(memory_space=pltpu.VMEM),) * 3,
        scratch_shapes=[
            pltpu.VMEM((2, 3, 10, 16, 128), I32),
            vm(8, 3, dtype=I32), vm(8, 4, dtype=I32), vm(6, dtype=I32), vm(4, dtype=I32), vm(4, dtype=I32), vm(dtype=I32),
            vm(8, 4), vm(8, 4), vm(8, 4),
            vm(6), vm(6), vm(4), vm(4), vm(4),
            vm(4), vm(4), vm(4), vm(), vm(),
            vm(8, 8, 4), vm(8, 6), vm(8, 4), vm(8, 4), vm(8, 4), vm(8), vm(8),
            vm(8, 6, 4), vm(8, 4), vm(8, 4),
            vm(3), vm(2), pltpu.VMEM((64, 128), F32), vm(),
            dma((2,)), dma((38,)), dma((38,)), dma((32,)), dma((64,)), dma((16,)), dma((16,)),
        ],
        compiler_params=pltpu.CompilerParams(
            collective_id=0, has_side_effects=True, vmem_limit_bytes=24 * 1024 * 1024
        ),
    )(pltpu.with_memory_space_constraint(probe_bits, pltpu.HBM), pltpu.with_memory_space_constraint(disorder_levels, pltpu.HBM))
    return pl.pallas_call(
        write_out,
        out_shape=shapes,
        in_specs=[pl.BlockSpec(memory_space=pltpu.VMEM)] * 3,
        out_specs=(pl.BlockSpec(memory_space=pltpu.HBM),) * 3,
        scratch_shapes=[dma((3,))],
        compiler_params=pltpu.CompilerParams(vmem_limit_bytes=4 * 1024 * 1024),
    )(*held)


def solution(mesh):
    return jax.shard_map(
        per_device,
        mesh=mesh,
        in_specs=(P("gx", "gz", "gy"), P("gx", "gz", "gy")),
        out_specs=(P(), P(None, "gx", "gz", "gy"), P(None, "gx", "gz", "gy")),
        check_vma=False,
    )
```

```python
import jax
import jax.numpy as jnp
from jax import lax
from jax.experimental import pallas as pl
from jax.experimental.pallas import tpu as pltpu
from jax.sharding import PartitionSpec as P

F32 = jnp.float32
I32 = jnp.int32
MESH = pl.DeviceIdType.MESH
C2 = 2.0 / 8.4
NSITES = 32 * 512 * 512
LOCAL = 4 * 32 * 128

DIRS = sorted(
    [
        (dx, dy, dz)
        for dx in (-1, 0, 1)
        for dy in (-1, 0, 1)
        for dz in (-1, 0, 1)
        if (dx, dy, dz) != (0, 0, 0)
    ],
    key=lambda d: (-abs(d[2]), abs(d[0]) + abs(d[1])),
)


def srl(a, n):
    return lax.shift_right_logical(a, n if hasattr(n, "shape") and n.shape == a.shape else jnp.full(a.shape, n, I32))


def roll(a, n, axis):
    return pltpu.roll(a, n % a.shape[axis], axis)


def add_counts(s1, c1, s2, c2):
    h = s1 & s2
    z = c1 ^ c2
    return s1 ^ s2, z ^ h, (c1 & c2) | (h & z)


def nibbles(planes, word, shift):
    ones = 0x11111111
    p0, p1, p2 = planes
    return (
        (srl(p0, shift) & ones)
        | ((srl(p1, shift) & ones) << 1)
        | ((srl(p2, shift) & ones) << 2)
        | ((srl(word, shift) & ones) << 3)
    )


def kernel(
    bits_hbm, dis_hbm, mom, prev, cur,
    E, LAT, NM, NZ1, NZ2, NY, NY2,
    EPM, EMM, E2M, EPZ1, EMZ1, EPZ2, EMZ2, E2Z, EPY, EMY, E2Y, EPY2, EMY2,
    V1M, V1Z1, V1Z2, V1Y, V1YI, V1Y2I, V1Y2, V2M, V2Z, V2YI, ACC, S, GP, GL,
    in_sem, hs, hr, ps, pr, ls, lr,
):
    gx, gy, gz = lax.axis_index("gx"), lax.axis_index("gy"), lax.axis_index("gz")
    yy, xhi = gz // 2, lax.rem(gz, 2)

    own_copies = [
        pltpu.make_async_copy(src, E.at[a, 1, 3:7, 0:8, :], in_sem.at[a])
        for a, src in enumerate((bits_hbm, dis_hbm))
    ]
    for cp in own_copies:
        cp.start()

    near_x = {d: lax.rem(gx + d + 8, 8) if d else gx for d in (-1, 0, 1)}
    near_y = {d: lax.rem(gy + d + 4, 4) if d else gy for d in (-1, 0, 1)}
    near_z = {d: lax.rem(gz + d + 16, 16) if d else gz for d in (-1, 0, 1)}

    def neighbour(d):
        return {"gx": near_x[d[0]], "gy": near_y[d[1]], "gz": near_z[d[2]]}

    core = lax.rem(gy, 2)
    pair = gy - core
    px = xhi * 2 + gy // 2
    place = yy * 4 + px
    line = [gx] + [lax.rem(gx + k, 8) for k in range(1, 8)]
    row_y = [yy * 2] + [lax.rem(yy + k, 8) * 2 for k in range(1, 8)]
    row_x = [px] + [lax.rem(px + k, 4) for k in range(1, 4)]
    row_h = [q // 2 for q in row_x]
    row_p = [(q - 2 * h) * 2 for q, h in zip(row_x, row_h)]

    def plane_peer(k, c):
        return {"gx": gx, "gy": row_p[k % 4] + c, "gz": row_y[k // 4] + row_h[k % 4]}

    def line_peer(k, c):
        return {"gx": line[k], "gy": pair + c, "gz": gz}

    barrier = pltpu.get_barrier_semaphore()

    def greet(device):
        pl.semaphore_signal(barrier, inc=1, device_id=device, device_id_type=MESH)

    for d in DIRS:
        greet(neighbour(d))
    for k in range(1, 8):
        greet(line_peer(k, 1))

    @pl.when(core == 0)
    def _():
        greet(line_peer(0, 1))

    @pl.when(core == 1)
    def _():
        for k in range(1, 32):
            greet(plane_peer(k, 1))

    lane = lax.broadcasted_iota(I32, (8, 128), 1)
    row = lax.broadcasted_iota(I32, (8, 128), 0)
    l0, l127 = lane == 0, lane == 127
    r0, r7 = row == 0, row == 7

    for cp in own_copies:
        cp.wait()

    @pl.when(core == 0)
    def _():
        pl.semaphore_wait(barrier, 26)

    @pl.when(core == 1)
    def _():
        pl.semaphore_wait(barrier, 26 + 31 + 15)


    def halo_copy(i, d, lo, hi):
        dx, dy, dz = d
        if dx == 1:
            xs, xd = slice(7 - hi, 7 - lo), slice(3 - hi, 3 - lo)
        elif dx == -1:
            xs, xd = slice(3 + lo, 3 + hi), slice(7 + lo, 7 + hi)
        else:
            xs, xd = slice(3, 7), slice(3, 7)
        if dz == 1:
            ws, wd = slice(7, 8), slice(15, 16)
        elif dz == -1:
            ws, wd = slice(0, 1), slice(8, 9)
        else:
            ws, wd = slice(0, 8), slice(0, 8)
        return pltpu.make_async_remote_copy(
            src_ref=E.at[:, 1, xs, ws, :],
            dst_ref=E.at[:, 1 - dy, xd, wd, :],
            send_sem=hs.at[i],
            recv_sem=hr.at[i],
            device_id=neighbour(d),
            device_id_type=MESH,
        )

    first, rest = [], []
    for d in DIRS:
        depth = 2 - abs(d[1]) - abs(d[2])
        if d[0] == 0 or depth > 0:
            first.append((d, halo_copy(len(first), d, 0, depth)))
    for d in DIRS:
        depth = 2 - abs(d[1]) - abs(d[2])
        if d[0] != 0:
            rest.append((d, halo_copy(len(first) + len(rest), d, depth, depth + 1)))
    for d, cp in first + rest:
        cp.start()
    for d, cp in first:
        if d[2] == 0:
            cp.wait_recv()

    def tile(a, t, xi, second):
        return E[a, t, xi + 1, (8 if second else 0) : (16 if second else 8), :]

    def pack_y(a, second, span):
        out = jnp.zeros((8, 128), I32)
        for xi in span:
            left, own, right = (tile(a, t, xi, second) for t in range(3))
            m1 = jnp.where(lane >= 64, left, own)
            m2 = jnp.where(lane >= 64, own, right)
            slot = lane - 16 * xi
            out = jnp.where((slot >= 0) & (slot < 8), roll(m1, 16 * xi - 125, 1), out)
            out = jnp.where((slot >= 8) & (slot < 16), roll(m2, 16 * xi + 8 - 126, 1), out)
        return out

    def up_down(main, second):
        up = roll(jnp.where(r0, second, main), 7, 0)
        down = roll(jnp.where(r7, second, main), 1, 0)
        return up, down

    def z_words(word, up, down):
        zp = (srl(word, 1) & 0x77777777) | (up << 3 & -0x77777778)
        zm = (word << 1 & -0x11111112) | (srl(down, 3) & 0x11111111)
        return zp, zm

    def sides(a, xi, second):
        left, own, right = (tile(a, t, xi, second) for t in range(3))
        return roll(jnp.where(l127, left, own), 1, 1), roll(jnp.where(l0, right, own), 127, 1)

    def energy(word, shift):
        return (srl(word, shift) & 255).astype(F32)

    def zshift(depth, unit):
        return jnp.where(row < 4, unit * (depth - 1), unit * (4 - depth))

    def weights(word, shift):
        lev = energy(word, shift)
        half = lev * (1.0 / 128.0)
        return half + (3.0 - 255.0 / 256.0 - 8.0), (3.0 + 255.0 / 256.0) - half

    def slope(word, shift):
        return energy(word, shift) * (C2 / 64.0) - (C2 * 255.0 / 128.0)

    def half_count(a, b, c):
        x = a ^ b
        return x ^ c, (a & b) | (c & x)

    def main_near(xi):
        dis = tile(1, 1, xi, False)
        for j in range(4):
            EPM[xi, j], EMM[xi, j] = weights(dis, 8 * j)
        ym, yp = sides(0, xi, False)
        LAT[xi, 0], LAT[xi, 1] = half_count(tile(0, 1, xi + 1, False), tile(0, 1, xi - 1, False), yp)
        LAT[xi, 2] = ym

    def main_slope(xi):
        for j in range(4):
            E2M[xi, j] = slope(tile(1, 1, xi, False), 8 * j)

    def main_words(xi):
        main, second = tile(0, 1, xi, False), tile(0, 1, xi, True)
        zp, zm = z_words(main, *up_down(main, second))
        planes = add_counts(LAT[xi, 0], LAT[xi, 1], *half_count(LAT[xi, 2], zp, zm))
        for j in range(4):
            NM[xi, j] = nibbles(planes, main, j)

    def edge_words(xi, shallow, deep):
        main, second = tile(0, 1, xi, False), tile(0, 1, xi, True)
        zp, zm = z_words(second, *up_down(second, main))
        ym, yp = sides(0, xi, True)
        dis = tile(1, 1, xi, True)
        planes = add_counts(
            *half_count(tile(0, 1, xi + 1, True), tile(0, 1, xi - 1, True), yp),
            *half_count(ym, zp, zm),
        )
        if shallow:
            NZ1[xi - 1] = nibbles(planes, second, zshift(1, 1))
            EPZ1[xi - 1], EMZ1[xi - 1] = weights(dis, zshift(1, 8))
        if deep:
            E2Z[xi - 2] = slope(dis, zshift(1, 8))
            NZ2[xi - 2] = nibbles(planes, second, zshift(2, 1))
            EPZ2[xi - 2], EMZ2[xi - 2] = weights(dis, zshift(2, 8))

    def y_planes(word, up, down):
        zp, zm = z_words(word, up, down)
        return add_counts(
            *half_count(roll(word, 1, 1), roll(word, 127, 1), roll(word, 16, 1)),
            *half_count(roll(word, 112, 1), zp, zm),
        )

    def y_words(yw, yw2):
        planes = y_planes(yw, *up_down(yw, yw2))
        for j in range(4):
            NY[j] = nibbles(planes, yw, j)

    def y_weights(yd):
        for j in range(4):
            EPY[j], EMY[j] = weights(yd, 8 * j)

    for xi in range(1, 7):
        main_near(xi)
    for xi in range(2, 6):
        main_slope(xi)
    yw = pack_y(0, False, range(1, 7))
    y_weights(pack_y(1, False, range(1, 7)))

    for d, cp in first:
        if d[2] != 0:
            cp.wait_recv()

    for xi in range(1, 7):
        main_words(xi)
    for xi in range(2, 6):
        edge_words(xi, True, False)
    y_words(yw, pack_y(0, True, range(2, 6)))

    col = lane & 15

    def inner(y):
        return jnp.where(col == 1, roll(y, 119, 1), y)

    def top(word, sh):
        return word << jnp.full(word.shape, sh, I32)

    def first_order(word, ep, em, sh):
        t = top(word, sh)
        q = lax.shift_right_arithmetic(t, jnp.full(t.shape, 28, I32)).astype(F32)
        return jnp.where(t < 0, ep, em) - q

    def sign(word, sh):
        return jnp.where(top(word, sh) < 0, 1.0, -1.0).astype(F32)

    def around(get, edge, ins, xi, j):
        c = get(xi, j)
        a = roll(ins, 0 - (16 * xi + 2), 1)
        s = get(xi + 1, j) + get(xi - 1, j)
        s = s + (jnp.where(l0, a, roll(c, 1, 1)) + jnp.where(l127, a, roll(c, 127, 1)))
        zp = get(xi, j + 1) if j < 3 else roll(jnp.where(r0, edge(xi), get(xi, 0)), 7, 0)
        zm = get(xi, j - 1) if j > 0 else roll(jnp.where(r7, edge(xi), get(xi, 3)), 1, 0)
        return c, s + (zp + zm)

    def second_main(r, xi, j, sg):
        c, s = around(lambda x, k: V1M[r, x, k], lambda x: V1Z1[r, x - 1], V1YI[r, j], xi, j)
        return c, (E2M[xi, j] * c - C2 * s) * C2 - sg

    def main_first(r, xi, sh):
        for j in range(4):
            V1M[r, xi, j] = first_order(NM[xi, j], EPM[xi, j], EMM[xi, j], sh)

    def edge_first(r, xi, sh):
        V1Z1[r, xi - 1] = first_order(NZ1[xi - 1], EPZ1[xi - 1], EMZ1[xi - 1], sh)

    def y_first(r, sh):
        for j in range(4):
            y = first_order(NY[j], EPY[j], EMY[j], sh)
            V1Y[r, j] = y
            V1YI[r, j] = inner(y)

    def pass_a1(r):
        sh = 28 - 4 * r
        for xi in range(2, 7):
            main_first(r, xi, sh)
        for xi in range(2, 6):
            edge_first(r, xi, sh)
        y_first(r, sh)

    def pass_a3(r):
        sh = 28 - 4 * r
        for xi in (0, 1, 7):
            main_first(r, xi, sh)
        for xi in (1, 6):
            edge_first(r, xi, sh)
        for xi in range(4):
            V1Z2[r, xi] = first_order(NZ2[xi], EPZ2[xi], EMZ2[xi], sh)
        y_first(r, sh)
        y = first_order(NY2[...], EPY2[...], EMY2[...], sh)
        V1Y2[r] = y
        V1Y2I[r] = inner(y)

    def moments_of(r):
        sh = 28 - 4 * r
        own = jnp.zeros((8, 128), F32)
        square = jnp.zeros((8, 128), F32)
        onsite = jnp.zeros((8, 128), F32)
        bonds = jnp.zeros((8, 128), F32)
        for xi in range(2, 6):
            for j in range(4):
                c = V1M[r, xi, j]
                side = roll(V1YI[r, j], 0 - (16 * xi + 2), 1)
                above = V1M[r, xi, j + 1] if j < 3 else roll(jnp.where(r0, V1Z1[r, xi - 1], V1M[r, xi, 0]), 7, 0)
                ahead = V1M[r, xi + 1, j] + jnp.where(l127, side, roll(c, 127, 1)) + above
                c2 = c * c
                own = own + jnp.where(top(NM[xi, j], sh) < 0, c, 0.0 - c)
                square = square + c2
                onsite = onsite + E2M[xi, j] * c2
                bonds = bonds + c * ahead
        m3 = (2.0 * C2 * C2) * (onsite - (2.0 * C2) * bonds) - (3.0 * C2) * own
        m2 = (2.0 * C2 * C2) * square - float(LOCAL // 1024)
        for m, acc in enumerate((C2 * own, m2, m3)):
            ACC[m, pl.ds(r, 1), :] = jnp.sum(acc, axis=0, keepdims=True)

    def pass_a2(r):
        sh = 28 - 4 * r
        for x in range(4):
            for j in range(4):
                v2 = second_main(r, x + 2, j, sign(NM[x + 2, j], sh))[1]
                V2M[r, x + 1, j] = v2
                prev[r, x, pl.ds(j, 8, stride=4), :] = v2

    def probes(one, group):
        def body(g, carry):
            for i in range(group):
                one(g * group + i)
            return carry

        lax.fori_loop(0, 8 // group, body, 0)

    probes(pass_a1, 8)
    probes(moments_of, 8)

    mine = jnp.zeros((8, 128), F32)
    for m in range(3):
        tot = jnp.sum(ACC[m], axis=1, keepdims=True)
        mine = mine + jnp.where(lane == row + 8 * m, jnp.broadcast_to(tot, (8, 128)), 0.0)

    def sum_rows(t):
        t = t + roll(t, 4, 0)
        t = t + roll(t, 2, 0)
        return t + roll(t, 1, 0)

    mine = sum_rows(mine)

    def plane_copy(k):
        return pltpu.make_async_remote_copy(
            src_ref=S.at[0, 0:1, :],
            dst_ref=GP.at[pl.ds(place, 1), :] if k else GP.at[32:33, :],
            send_sem=ps.at[k],
            recv_sem=pr.at[k],
            device_id=plane_peer(k, 1),
            device_id_type=MESH,
        )

    def line_copy(k, c):
        return pltpu.make_async_remote_copy(
            src_ref=S.at[1, 0:1, :],
            dst_ref=GL.at[pl.ds(gx, 1), :],
            send_sem=ls.at[c * 8 + k],
            recv_sem=lr.at[c * 8 + k],
            device_id=line_peer(k, c),
            device_id_type=MESH,
        )

    S[0] = mine

    @pl.when(core == 0)
    def _():
        plane_copy(0).start()

    @pl.when(core == 1)
    def _():
        plane_copy(0).wait_recv()
        S[0] = mine + GP[32:33, :]
        for k in range(1, 32):
            plane_copy(k).start()


    for d, cp in rest:
        cp.wait_recv()
    for xi in (0, 7):
        main_near(xi)
        main_words(xi)
    for xi in (1, 6):
        main_slope(xi)
        edge_words(xi, True, False)
    for xi in range(2, 6):
        edge_words(xi, False, True)
    yw, yw2 = pack_y(0, False, range(8)), pack_y(0, True, range(8))
    yd, yd2 = pack_y(1, False, range(8)), pack_y(1, True, range(8))
    y_words(yw, yw2)
    y_weights(yd)
    for j in range(4):
        E2Y[j] = slope(yd, 8 * j)
    NY2[...] = nibbles(y_planes(yw2, *up_down(yw2, yw)), yw2, zshift(1, 1))
    EPY2[...], EMY2[...] = weights(yd2, zshift(1, 8))
    probes(pass_a3, 2)
    probes(pass_a2, 4)

    def pass_b(r):
        sh = 28 - 4 * r
        for xi, slot2 in ((1, 0), (6, 5)):
            for j in range(4):
                V2M[r, slot2, j] = second_main(r, xi, j, sign(NM[xi, j], sh))[1]
        for x in range(4):
            xi = x + 2
            c = V1Z1[r, xi - 1]
            a = roll(V1Y2I[r], 0 - (16 * xi + 2), 1)
            s = V1Z1[r, xi] + V1Z1[r, xi - 2]
            s = s + (jnp.where(l0, a, roll(c, 1, 1)) + jnp.where(l127, a, roll(c, 127, 1)))
            ins = jnp.where(r7, roll(V1M[r, xi, 0], 7, 0), roll(V1M[r, xi, 3], 1, 0))
            s = s + (V1Z2[r, x] + ins)
            V2Z[r, x] = (E2Z[x] * c - C2 * s) * C2 - sign(NZ1[xi - 1], sh)
        for j in range(4):
            c = V1Y[r, j]
            s = roll(c, 1, 1) + roll(c, 127, 1) + (roll(c, 16, 1) + roll(c, 112, 1))
            zp = V1Y[r, j + 1] if j < 3 else roll(jnp.where(r0, V1Y2[r], V1Y[r, 0]), 7, 0)
            zm = V1Y[r, j - 1] if j > 0 else roll(jnp.where(r7, V1Y2[r], V1Y[r, 3]), 1, 0)
            s = s + (zp + zm)
            V2YI[r, j] = inner((E2Y[j] * c - C2 * s) * C2 - sign(NY[j], sh))

    def pass_c(r):
        for x in range(4):
            for j in range(4):
                c, s = around(
                    lambda xi, k: V2M[r, xi - 1, k], lambda xi: V2Z[r, xi - 2], V2YI[r, j], x + 2, j
                )
                v3 = E2M[x + 2, j] * c - C2 * s - C2 * V1M[r, x + 2, j]
                cur[r, x, pl.ds(j, 8, stride=4), :] = v3

    probes(pass_b, 2)
    probes(pass_c, 4)

    @pl.when(core == 1)
    def _():
        for k in range(1, 32):
            plane_copy(k).wait_recv()
        acc = jnp.zeros((8, 128), F32)
        for q in range(4):
            acc = acc + jnp.where(row + 8 * q == place, S[0], GP[8 * q : 8 * q + 8, :])
        S[1] = sum_rows(acc)
        for k in range(8):
            line_copy(k, 0).start()
        for k in range(1, 8):
            line_copy(k, 1).start()
        GL[pl.ds(gx, 1), :] = S[1, 0:1, :]

    for _, cp in first + rest:
        cp.wait_send()

    @pl.when(core == 0)
    def _():
        plane_copy(0).wait_send()
        for k in range(8):
            line_copy(k, 0).wait_recv()

    @pl.when(core == 1)
    def _():
        for k in range(1, 32):
            plane_copy(k).wait_send()
        for k in range(1, 8):
            line_copy(k, 1).wait_recv()

    total = sum_rows(GL[...]) * (1.0 / NSITES)
    out = jnp.where(r0, total, jnp.where(row == 1, roll(total, 120, 1), roll(total, 112, 1)))
    mom[...] = out[:3, :8]

    @pl.when(core == 1)
    def _():
        for k in range(8):
            line_copy(k, 0).wait_send()
        for k in range(1, 8):
            line_copy(k, 1).wait_send()


def write_out(mom, prev, cur, mom_out, prev_out, cur_out, sems):
    copies = [
        pltpu.make_async_copy(src, dst, sems.at[i])
        for i, (src, dst) in enumerate(((prev, prev_out), (cur, cur_out), (mom, mom_out)))
    ]
    for cp in copies:
        cp.start()
    for cp in copies:
        cp.wait()


def vm(*shape, dtype=F32):
    return pltpu.VMEM(shape + (8, 128), dtype)


def per_device(probe_bits, disorder_levels):
    dma = pltpu.SemaphoreType.DMA
    shapes = (
        jax.ShapeDtypeStruct((3, 8), F32),
        jax.ShapeDtypeStruct((8, 4, 32, 128), F32),
        jax.ShapeDtypeStruct((8, 4, 32, 128), F32),
    )
    held = pl.pallas_call(
        kernel,
        out_shape=shapes,
        in_specs=[pl.BlockSpec(memory_space=pltpu.HBM)] * 2,
        out_specs=(pl.BlockSpec(memory_space=pltpu.VMEM),) * 3,
        scratch_shapes=[
            pltpu.VMEM((2, 3, 10, 16, 128), I32),
            vm(8, 3, dtype=I32), vm(8, 4, dtype=I32), vm(6, dtype=I32), vm(4, dtype=I32), vm(4, dtype=I32), vm(dtype=I32),
            vm(8, 4), vm(8, 4), vm(8, 4),
            vm(6), vm(6), vm(4), vm(4), vm(4),
            vm(4), vm(4), vm(4), vm(), vm(),
            vm(8, 8, 4), vm(8, 6), vm(8, 4), vm(8, 4), vm(8, 4), vm(8), vm(8),
            vm(8, 6, 4), vm(8, 4), vm(8, 4),
            vm(3), vm(2), pltpu.VMEM((40, 128), F32), vm(),
            dma((2,)), dma((38,)), dma((38,)), dma((32,)), dma((32,)), dma((16,)), dma((16,)),
        ],
        compiler_params=pltpu.CompilerParams(
            collective_id=0, has_side_effects=True, vmem_limit_bytes=24 * 1024 * 1024
        ),
    )(pltpu.with_memory_space_constraint(probe_bits, pltpu.HBM), pltpu.with_memory_space_constraint(disorder_levels, pltpu.HBM))
    return pl.pallas_call(
        write_out,
        out_shape=shapes,
        in_specs=[pl.BlockSpec(memory_space=pltpu.VMEM)] * 3,
        out_specs=(pl.BlockSpec(memory_space=pltpu.HBM),) * 3,
        scratch_shapes=[dma((3,))],
        compiler_params=pltpu.CompilerParams(vmem_limit_bytes=4 * 1024 * 1024),
    )(*held)


def solution(mesh):
    return jax.shard_map(
        per_device,
        mesh=mesh,
        in_specs=(P("gx", "gz", "gy"), P("gx", "gz", "gy")),
        out_specs=(P(), P(None, "gx", "gz", "gy"), P(None, "gx", "gz", "gy")),
        check_vma=False,
    )
```

```python
import jax
import jax.numpy as jnp
from jax import lax
from jax.experimental import pallas as pl
from jax.experimental.pallas import tpu as pltpu
from jax.sharding import PartitionSpec as P

F32 = jnp.float32
I32 = jnp.int32
MESH = pl.DeviceIdType.MESH
C2 = 2.0 / 8.4
NSITES = 32 * 512 * 512
LOCAL = 4 * 32 * 128

DIRS = sorted(
    [
        (dx, dy, dz)
        for dx in (-1, 0, 1)
        for dy in (-1, 0, 1)
        for dz in (-1, 0, 1)
        if (dx, dy, dz) != (0, 0, 0)
    ],
    key=lambda d: (-abs(d[2]), abs(d[0]) + abs(d[1])),
)


def srl(a, n):
    return lax.shift_right_logical(a, n if hasattr(n, "shape") and n.shape == a.shape else jnp.full(a.shape, n, I32))


def roll(a, n, axis):
    return pltpu.roll(a, n % a.shape[axis], axis)


def add_counts(s1, c1, s2, c2):
    h = s1 & s2
    z = c1 ^ c2
    return s1 ^ s2, z ^ h, (c1 & c2) | (h & z)


def nibbles(planes, word, shift):
    ones = 0x11111111
    p0, p1, p2 = planes
    return (
        (srl(p0, shift) & ones)
        | ((srl(p1, shift) & ones) << 1)
        | ((srl(p2, shift) & ones) << 2)
        | ((srl(word, shift) & ones) << 3)
    )


def kernel(
    bits_hbm, dis_hbm, mom, prev, cur,
    E, LAT, NM, NZ1, NZ2, NY, NY2,
    EPM, EMM, E2M, EPZ1, EMZ1, EPZ2, EMZ2, E2Z, EPY, EMY, E2Y, EPY2, EMY2,
    V1M, V1Z1, V1Z2, V1Y, V1YI, V1Y2I, V1Y2, V2M, V2Z, V2YI, ACC, S, GP, GL,
    in_sem, hs, hr, ps, pr, ls, lr,
):
    gx, gy, gz = lax.axis_index("gx"), lax.axis_index("gy"), lax.axis_index("gz")
    yy, xhi = gz // 2, lax.rem(gz, 2)

    own_copies = [
        pltpu.make_async_copy(src, E.at[a, 1, 3:7, 0:8, :], in_sem.at[a])
        for a, src in enumerate((bits_hbm, dis_hbm))
    ]
    for cp in own_copies:
        cp.start()

    near_x = {d: lax.rem(gx + d + 8, 8) if d else gx for d in (-1, 0, 1)}
    near_y = {d: lax.rem(gy + d + 4, 4) if d else gy for d in (-1, 0, 1)}
    near_z = {d: lax.rem(gz + d + 16, 16) if d else gz for d in (-1, 0, 1)}

    def neighbour(d):
        return {"gx": near_x[d[0]], "gy": near_y[d[1]], "gz": near_z[d[2]]}

    core = lax.rem(gy, 2)
    pair = gy - core
    px = xhi * 2 + gy // 2
    place = yy * 4 + px
    line = [gx] + [lax.rem(gx + k, 8) for k in range(1, 8)]
    row_y = [yy * 2] + [lax.rem(yy + k, 8) * 2 for k in range(1, 8)]
    row_x = [px] + [lax.rem(px + k, 4) for k in range(1, 4)]
    row_h = [q // 2 for q in row_x]
    row_p = [(q - 2 * h) * 2 for q, h in zip(row_x, row_h)]

    def plane_peer(k, c):
        return {"gx": gx, "gy": row_p[k % 4] + c, "gz": row_y[k // 4] + row_h[k % 4]}

    def line_peer(k, c):
        return {"gx": line[k], "gy": pair + c, "gz": gz}

    barrier = pltpu.get_barrier_semaphore()

    def greet(device):
        pl.semaphore_signal(barrier, inc=1, device_id=device, device_id_type=MESH)

    for d in DIRS:
        greet(neighbour(d))
    for k in range(1, 8):
        greet(line_peer(k, 1))

    @pl.when(core == 0)
    def _():
        greet(line_peer(0, 1))

    @pl.when(core == 1)
    def _():
        for k in range(1, 32):
            greet(plane_peer(k, 1))
        for k in range(32):
            greet(plane_peer(k, 0))

    lane = lax.broadcasted_iota(I32, (8, 128), 1)
    row = lax.broadcasted_iota(I32, (8, 128), 0)
    l0, l127 = lane == 0, lane == 127
    r0, r7 = row == 0, row == 7

    for cp in own_copies:
        cp.wait()

    @pl.when(core == 0)
    def _():
        pl.semaphore_wait(barrier, 26 + 32)

    @pl.when(core == 1)
    def _():
        pl.semaphore_wait(barrier, 26 + 31 + 15)


    def halo_copy(i, d, lo, hi):
        dx, dy, dz = d
        if dx == 1:
            xs, xd = slice(7 - hi, 7 - lo), slice(3 - hi, 3 - lo)
        elif dx == -1:
            xs, xd = slice(3 + lo, 3 + hi), slice(7 + lo, 7 + hi)
        else:
            xs, xd = slice(3, 7), slice(3, 7)
        if dz == 1:
            ws, wd = slice(7, 8), slice(15, 16)
        elif dz == -1:
            ws, wd = slice(0, 1), slice(8, 9)
        else:
            ws, wd = slice(0, 8), slice(0, 8)
        return pltpu.make_async_remote_copy(
            src_ref=E.at[:, 1, xs, ws, :],
            dst_ref=E.at[:, 1 - dy, xd, wd, :],
            send_sem=hs.at[i],
            recv_sem=hr.at[i],
            device_id=neighbour(d),
            device_id_type=MESH,
        )

    first, rest = [], []
    for d in DIRS:
        depth = 2 - abs(d[1]) - abs(d[2])
        if d[0] == 0 or depth > 0:
            first.append((d, halo_copy(len(first), d, 0, depth)))
    for d in DIRS:
        depth = 2 - abs(d[1]) - abs(d[2])
        if d[0] != 0:
            rest.append((d, halo_copy(len(first) + len(rest), d, depth, depth + 1)))
    for d, cp in first + rest:
        cp.start()
    for d, cp in first:
        if d[2] == 0:
            cp.wait_recv()

    def tile(a, t, xi, second):
        return E[a, t, xi + 1, (8 if second else 0) : (16 if second else 8), :]

    def pack_y(a, second, span):
        out = jnp.zeros((8, 128), I32)
        for xi in span:
            left, own, right = (tile(a, t, xi, second) for t in range(3))
            m1 = jnp.where(lane >= 64, left, own)
            m2 = jnp.where(lane >= 64, own, right)
            slot = lane - 16 * xi
            out = jnp.where((slot >= 0) & (slot < 8), roll(m1, 16 * xi - 125, 1), out)
            out = jnp.where((slot >= 8) & (slot < 16), roll(m2, 16 * xi + 8 - 126, 1), out)
        return out

    def up_down(main, second):
        up = roll(jnp.where(r0, second, main), 7, 0)
        down = roll(jnp.where(r7, second, main), 1, 0)
        return up, down

    def z_words(word, up, down):
        zp = (srl(word, 1) & 0x77777777) | (up << 3 & -0x77777778)
        zm = (word << 1 & -0x11111112) | (srl(down, 3) & 0x11111111)
        return zp, zm

    def sides(a, xi, second):
        left, own, right = (tile(a, t, xi, second) for t in range(3))
        return roll(jnp.where(l127, left, own), 1, 1), roll(jnp.where(l0, right, own), 127, 1)

    def energy(word, shift):
        return (srl(word, shift) & 255).astype(F32)

    def zshift(depth, unit):
        return jnp.where(row < 4, unit * (depth - 1), unit * (4 - depth))

    def weights(word, shift):
        lev = energy(word, shift)
        half = lev * (1.0 / 128.0)
        return half + (3.0 - 255.0 / 256.0 - 8.0), (3.0 + 255.0 / 256.0) - half

    def slope(word, shift):
        return energy(word, shift) * (C2 / 64.0) - (C2 * 255.0 / 128.0)

    def half_count(a, b, c):
        x = a ^ b
        return x ^ c, (a & b) | (c & x)

    def main_near(xi):
        dis = tile(1, 1, xi, False)
        for j in range(4):
            EPM[xi, j], EMM[xi, j] = weights(dis, 8 * j)
        ym, yp = sides(0, xi, False)
        LAT[xi, 0], LAT[xi, 1] = half_count(tile(0, 1, xi + 1, False), tile(0, 1, xi - 1, False), yp)
        LAT[xi, 2] = ym

    def main_slope(xi):
        for j in range(4):
            E2M[xi, j] = slope(tile(1, 1, xi, False), 8 * j)

    def main_words(xi):
        main, second = tile(0, 1, xi, False), tile(0, 1, xi, True)
        zp, zm = z_words(main, *up_down(main, second))
        planes = add_counts(LAT[xi, 0], LAT[xi, 1], *half_count(LAT[xi, 2], zp, zm))
        for j in range(4):
            NM[xi, j] = nibbles(planes, main, j)

    def edge_words(xi, shallow, deep):
        main, second = tile(0, 1, xi, False), tile(0, 1, xi, True)
        zp, zm = z_words(second, *up_down(second, main))
        ym, yp = sides(0, xi, True)
        dis = tile(1, 1, xi, True)
        planes = add_counts(
            *half_count(tile(0, 1, xi + 1, True), tile(0, 1, xi - 1, True), yp),
            *half_count(ym, zp, zm),
        )
        if shallow:
            NZ1[xi - 1] = nibbles(planes, second, zshift(1, 1))
            EPZ1[xi - 1], EMZ1[xi - 1] = weights(dis, zshift(1, 8))
        if deep:
            E2Z[xi - 2] = slope(dis, zshift(1, 8))
            NZ2[xi - 2] = nibbles(planes, second, zshift(2, 1))
            EPZ2[xi - 2], EMZ2[xi - 2] = weights(dis, zshift(2, 8))

    def y_planes(word, up, down):
        zp, zm = z_words(word, up, down)
        return add_counts(
            *half_count(roll(word, 1, 1), roll(word, 127, 1), roll(word, 16, 1)),
            *half_count(roll(word, 112, 1), zp, zm),
        )

    def y_words(yw, yw2):
        planes = y_planes(yw, *up_down(yw, yw2))
        for j in range(4):
            NY[j] = nibbles(planes, yw, j)

    def y_weights(yd):
        for j in range(4):
            EPY[j], EMY[j] = weights(yd, 8 * j)

    for xi in range(1, 7):
        main_near(xi)
    for xi in range(2, 6):
        main_slope(xi)
    yw = pack_y(0, False, range(1, 7))
    y_weights(pack_y(1, False, range(1, 7)))

    for d, cp in first:
        if d[2] != 0:
            cp.wait_recv()

    for xi in range(1, 7):
        main_words(xi)
    for xi in range(2, 6):
        edge_words(xi, True, False)
    y_words(yw, pack_y(0, True, range(2, 6)))

    col = lane & 15

    def inner(y):
        return jnp.where(col == 1, roll(y, 119, 1), y)

    def top(word, sh):
        return word << jnp.full(word.shape, sh, I32)

    def first_order(word, ep, em, sh):
        t = top(word, sh)
        q = lax.shift_right_arithmetic(t, jnp.full(t.shape, 28, I32)).astype(F32)
        return jnp.where(t < 0, ep, em) - q

    def sign(word, sh):
        return jnp.where(top(word, sh) < 0, 1.0, -1.0).astype(F32)

    def around(get, edge, ins, xi, j):
        c = get(xi, j)
        a = roll(ins, 0 - (16 * xi + 2), 1)
        s = get(xi + 1, j) + get(xi - 1, j)
        s = s + (jnp.where(l0, a, roll(c, 1, 1)) + jnp.where(l127, a, roll(c, 127, 1)))
        zp = get(xi, j + 1) if j < 3 else roll(jnp.where(r0, edge(xi), get(xi, 0)), 7, 0)
        zm = get(xi, j - 1) if j > 0 else roll(jnp.where(r7, edge(xi), get(xi, 3)), 1, 0)
        return c, s + (zp + zm)

    def second_main(r, xi, j, sg):
        c, s = around(lambda x, k: V1M[r, x, k], lambda x: V1Z1[r, x - 1], V1YI[r, j], xi, j)
        return c, (E2M[xi, j] * c - C2 * s) * C2 - sg

    def main_first(r, xi, sh):
        for j in range(4):
            V1M[r, xi, j] = first_order(NM[xi, j], EPM[xi, j], EMM[xi, j], sh)

    def edge_first(r, xi, sh):
        V1Z1[r, xi - 1] = first_order(NZ1[xi - 1], EPZ1[xi - 1], EMZ1[xi - 1], sh)

    def y_first(r, sh):
        for j in range(4):
            y = first_order(NY[j], EPY[j], EMY[j], sh)
            V1Y[r, j] = y
            V1YI[r, j] = inner(y)

    def pass_a1(r):
        sh = 28 - 4 * r
        for xi in range(2, 7):
            main_first(r, xi, sh)
        for xi in range(2, 6):
            edge_first(r, xi, sh)
        y_first(r, sh)

    def pass_a3(r):
        sh = 28 - 4 * r
        for xi in (0, 1, 7):
            main_first(r, xi, sh)
        for xi in (1, 6):
            edge_first(r, xi, sh)
        for xi in range(4):
            V1Z2[r, xi] = first_order(NZ2[xi], EPZ2[xi], EMZ2[xi], sh)
        y_first(r, sh)
        y = first_order(NY2[...], EPY2[...], EMY2[...], sh)
        V1Y2[r] = y
        V1Y2I[r] = inner(y)

    def moments_of(r):
        sh = 28 - 4 * r
        own = jnp.zeros((8, 128), F32)
        square = jnp.zeros((8, 128), F32)
        onsite = jnp.zeros((8, 128), F32)
        bonds = jnp.zeros((8, 128), F32)
        for xi in range(2, 6):
            for j in range(4):
                c = V1M[r, xi, j]
                side = roll(V1YI[r, j], 0 - (16 * xi + 2), 1)
                above = V1M[r, xi, j + 1] if j < 3 else roll(jnp.where(r0, V1Z1[r, xi - 1], V1M[r, xi, 0]), 7, 0)
                ahead = V1M[r, xi + 1, j] + jnp.where(l127, side, roll(c, 127, 1)) + above
                c2 = c * c
                own = own + jnp.where(top(NM[xi, j], sh) < 0, c, 0.0 - c)
                square = square + c2
                onsite = onsite + E2M[xi, j] * c2
                bonds = bonds + c * ahead
        m3 = (2.0 * C2 * C2) * (onsite - (2.0 * C2) * bonds) - (3.0 * C2) * own
        m2 = (2.0 * C2 * C2) * square - float(LOCAL // 1024)
        for m, acc in enumerate((C2 * own, m2, m3)):
            ACC[m, pl.ds(r, 1), :] = jnp.sum(acc, axis=0, keepdims=True)

    def pass_a2(r):
        sh = 28 - 4 * r
        for x in range(4):
            for j in range(4):
                v2 = second_main(r, x + 2, j, sign(NM[x + 2, j], sh))[1]
                V2M[r, x + 1, j] = v2
                prev[r, x, pl.ds(j, 8, stride=4), :] = v2

    def probes(one, group):
        def body(g, carry):
            for i in range(group):
                one(g * group + i)
            return carry

        lax.fori_loop(0, 8 // group, body, 0)

    probes(pass_a1, 8)
    probes(moments_of, 8)

    mine = jnp.zeros((8, 128), F32)
    for m in range(3):
        tot = jnp.sum(ACC[m], axis=1, keepdims=True)
        mine = mine + jnp.where(lane == row + 8 * m, jnp.broadcast_to(tot, (8, 128)), 0.0)

    def sum_rows(t):
        t = t + roll(t, 4, 0)
        t = t + roll(t, 2, 0)
        return t + roll(t, 1, 0)

    mine = sum_rows(mine)

    slot = place * 2 + core

    def plane_copy(k):
        return pltpu.make_async_remote_copy(
            src_ref=S.at[0, 0:1, :],
            dst_ref=GP.at[pl.ds(slot, 1), :],
            send_sem=ps.at[k],
            recv_sem=pr.at[(1 - core) * 32 + k],
            device_id=plane_peer(k, 1),
            device_id_type=MESH,
        )

    def line_copy(k, c):
        return pltpu.make_async_remote_copy(
            src_ref=S.at[1, 0:1, :],
            dst_ref=GL.at[pl.ds(gx, 1), :],
            send_sem=ls.at[c * 8 + k],
            recv_sem=lr.at[c * 8 + k],
            device_id=line_peer(k, c),
            device_id_type=MESH,
        )

    def plane_arrived(q):
        return pltpu.make_async_remote_copy(
            src_ref=S.at[0, 0:1, :],
            dst_ref=GP.at[0:1, :],
            send_sem=ps.at[0],
            recv_sem=pr.at[q],
            device_id=plane_peer(1, 1),
            device_id_type=MESH,
        ).wait_recv()

    S[0] = mine
    for k in range(1, 32):
        plane_copy(k).start()

    @pl.when(core == 0)
    def _():
        plane_copy(0).start()


    for d, cp in rest:
        cp.wait_recv()
    for xi in (0, 7):
        main_near(xi)
        main_words(xi)
    for xi in (1, 6):
        main_slope(xi)
        edge_words(xi, True, False)
    for xi in range(2, 6):
        edge_words(xi, False, True)
    yw, yw2 = pack_y(0, False, range(8)), pack_y(0, True, range(8))
    yd, yd2 = pack_y(1, False, range(8)), pack_y(1, True, range(8))
    y_words(yw, yw2)
    y_weights(yd)
    for j in range(4):
        E2Y[j] = slope(yd, 8 * j)
    NY2[...] = nibbles(y_planes(yw2, *up_down(yw2, yw)), yw2, zshift(1, 1))
    EPY2[...], EMY2[...] = weights(yd2, zshift(1, 8))
    probes(pass_a3, 2)
    probes(pass_a2, 4)

    def pass_b(r):
        sh = 28 - 4 * r
        for xi, slot2 in ((1, 0), (6, 5)):
            for j in range(4):
                V2M[r, slot2, j] = second_main(r, xi, j, sign(NM[xi, j], sh))[1]
        for x in range(4):
            xi = x + 2
            c = V1Z1[r, xi - 1]
            a = roll(V1Y2I[r], 0 - (16 * xi + 2), 1)
            s = V1Z1[r, xi] + V1Z1[r, xi - 2]
            s = s + (jnp.where(l0, a, roll(c, 1, 1)) + jnp.where(l127, a, roll(c, 127, 1)))
            ins = jnp.where(r7, roll(V1M[r, xi, 0], 7, 0), roll(V1M[r, xi, 3], 1, 0))
            s = s + (V1Z2[r, x] + ins)
            V2Z[r, x] = (E2Z[x] * c - C2 * s) * C2 - sign(NZ1[xi - 1], sh)
        for j in range(4):
            c = V1Y[r, j]
            s = roll(c, 1, 1) + roll(c, 127, 1) + (roll(c, 16, 1) + roll(c, 112, 1))
            zp = V1Y[r, j + 1] if j < 3 else roll(jnp.where(r0, V1Y2[r], V1Y[r, 0]), 7, 0)
            zm = V1Y[r, j - 1] if j > 0 else roll(jnp.where(r7, V1Y2[r], V1Y[r, 3]), 1, 0)
            s = s + (zp + zm)
            V2YI[r, j] = inner((E2Y[j] * c - C2 * s) * C2 - sign(NY[j], sh))

    def pass_c(r):
        for x in range(4):
            for j in range(4):
                c, s = around(
                    lambda xi, k: V2M[r, xi - 1, k], lambda xi: V2Z[r, xi - 2], V2YI[r, j], x + 2, j
                )
                v3 = E2M[x + 2, j] * c - C2 * s - C2 * V1M[r, x + 2, j]
                cur[r, x, pl.ds(j, 8, stride=4), :] = v3

    probes(pass_b, 2)
    probes(pass_c, 4)

    @pl.when(core == 1)
    def _():
        for q in range(1, 64):
            plane_arrived(q)
        acc = jnp.zeros((8, 128), F32)
        for q in range(8):
            acc = acc + jnp.where(row + 8 * q == slot, mine, GP[8 * q : 8 * q + 8, :])
        S[1] = sum_rows(acc)
        for k in range(8):
            line_copy(k, 0).start()
        for k in range(1, 8):
            line_copy(k, 1).start()
        GL[pl.ds(gx, 1), :] = S[1, 0:1, :]

    for _, cp in first + rest:
        cp.wait_send()
    for k in range(1, 32):
        plane_copy(k).wait_send()

    @pl.when(core == 0)
    def _():
        plane_copy(0).wait_send()
        for k in range(8):
            line_copy(k, 0).wait_recv()

    @pl.when(core == 1)
    def _():
        for k in range(1, 8):
            line_copy(k, 1).wait_recv()

    mom[...] = GL[...]

    @pl.when(core == 1)
    def _():
        for k in range(8):
            line_copy(k, 0).wait_send()
        for k in range(1, 8):
            line_copy(k, 1).wait_send()


def write_out(rows, prev, cur, mom_out, prev_out, cur_out, mom, sems):
    copies = [
        pltpu.make_async_copy(src, dst, sems.at[i])
        for i, (src, dst) in enumerate(((prev, prev_out), (cur, cur_out), (mom, mom_out)))
    ]
    for cp in copies[:2]:
        cp.start()
    row = lax.broadcasted_iota(I32, (8, 128), 0)
    total = jnp.broadcast_to(jnp.sum(rows[...], axis=0, keepdims=True), (8, 128)) * (1.0 / NSITES)
    out = jnp.where(row == 0, total, jnp.where(row == 1, roll(total, 120, 1), roll(total, 112, 1)))
    mom[...] = out[:3, :8]
    copies[2].start()
    for cp in copies:
        cp.wait()


def vm(*shape, dtype=F32):
    return pltpu.VMEM(shape + (8, 128), dtype)


def per_device(probe_bits, disorder_levels):
    dma = pltpu.SemaphoreType.DMA
    shapes = (
        jax.ShapeDtypeStruct((3, 8), F32),
        jax.ShapeDtypeStruct((8, 4, 32, 128), F32),
        jax.ShapeDtypeStruct((8, 4, 32, 128), F32),
    )
    held = pl.pallas_call(
        kernel,
        out_shape=(jax.ShapeDtypeStruct((8, 128), F32),) + shapes[1:],
        in_specs=[pl.BlockSpec(memory_space=pltpu.HBM)] * 2,
        out_specs=(pl.BlockSpec(memory_space=pltpu.VMEM),) * 3,
        scratch_shapes=[
            pltpu.VMEM((2, 3, 10, 16, 128), I32),
            vm(8, 3, dtype=I32), vm(8, 4, dtype=I32), vm(6, dtype=I32), vm(4, dtype=I32), vm(4, dtype=I32), vm(dtype=I32),
            vm(8, 4), vm(8, 4), vm(8, 4),
            vm(6), vm(6), vm(4), vm(4), vm(4),
            vm(4), vm(4), vm(4), vm(), vm(),
            vm(8, 8, 4), vm(8, 6), vm(8, 4), vm(8, 4), vm(8, 4), vm(8), vm(8),
            vm(8, 6, 4), vm(8, 4), vm(8, 4),
            vm(3), vm(2), pltpu.VMEM((64, 128), F32), vm(),
            dma((2,)), dma((38,)), dma((38,)), dma((32,)), dma((64,)), dma((16,)), dma((16,)),
        ],
        compiler_params=pltpu.CompilerParams(
            collective_id=0, has_side_effects=True, vmem_limit_bytes=24 * 1024 * 1024
        ),
    )(pltpu.with_memory_space_constraint(probe_bits, pltpu.HBM), pltpu.with_memory_space_constraint(disorder_levels, pltpu.HBM))
    return pl.pallas_call(
        write_out,
        out_shape=shapes,
        in_specs=[pl.BlockSpec(memory_space=pltpu.VMEM)] * 3,
        out_specs=(pl.BlockSpec(memory_space=pltpu.HBM),) * 3,
        scratch_shapes=[pltpu.VMEM((3, 8), F32), dma((3,))],
        compiler_params=pltpu.CompilerParams(vmem_limit_bytes=4 * 1024 * 1024),
    )(*held)


def solution(mesh):
    return jax.shard_map(
        per_device,
        mesh=mesh,
        in_specs=(P("gx", "gz", "gy"), P("gx", "gz", "gy")),
        out_specs=(P(), P(None, "gx", "gz", "gy"), P(None, "gx", "gz", "gy")),
        check_vma=False,
    )
```
